512 devices in a mesh: section: 8 (over y), dp: 64 (over x, z, core).
Axes of the slice: x: 4, y: 8, z: 8, core: 2. Of those that a mesh axis runs over, the one named last changes fastest.
Arguments:
- activations: bfloat16 [8, 4, 64, 14336], P('section', None, 'dp'), may hold values from -6 to 6
- out_grads: bfloat16 [8, 4, 64, 4096], P('section', None, 'dp'), may hold values from -6 to 6
- basis_in: bfloat16 [8, 14336, 1024], P('section', 'dp'), may hold values from -0.046875 to 0.046875
- basis_out: bfloat16 [8, 4096, 1024], P('section', 'dp'), may hold values from -0.09375 to 0.09375
- eigen_values: float32 [8, 1024, 1024], P('section', 'dp'), may hold values from 0.02 to 2
- query_proj: bfloat16 [8, 8, 1024, 1024], P('section', None, 'dp'), may hold values from -0.046875 to 0.046875
- lengths: int32 [4], replicated, may hold values from 16 to 64
- seq_rows: int32 [4], replicated, may hold values from 0 to 511
- prior_table: float32 [512, 8], P('dp'), may hold values from -6 to 6
Outputs:
- influence: float32 [8, 512, 8], P('section', 'dp')
The draws below stay inside these ranges and needn't reach their ends.
All inputs are finite; a program needn't handle non-finite values.
Results may differ from the reference program's by a relative error of at most 0.01.
Values may be sent and summed in bfloat16 or wider, within the bound.
A program may use at most 64 MiB of HBM per device.

```python
import math
import jax
import jax.numpy as jnp
from jax import lax

D = 4096
FFW = 14336
RANK = 1024
QUERIES = 8
MB = 4
SECTIONS = 8
SLOTS = 64
TABLE = 512


def with_ends(values, stream_key, low, largest):
    spot = [jax.random.randint(jax.random.fold_in(stream_key, axis), (), 0, length) for axis, length in enumerate(values.shape)]
    widest = values.shape.index(max(values.shape))
    neighbour = spot[:widest] + [(spot[widest] + 1) % values.shape[widest]] + spot[widest + 1:]
    return values.at[tuple(spot)].set(low).at[tuple(neighbour)].set(largest)


def shard_levels(key, dims, pieces, low, top_value):
    level = 1.0
    for dim, shards_of in pieces:
        steps = jax.random.uniform(jax.random.fold_in(jax.random.fold_in(key, 6), dim), (shards_of,), jnp.float32, low / len(pieces), top_value / len(pieces))
        level = level * jnp.repeat(jnp.exp(steps), dims[dim] // shards_of).reshape((-1,) + (1,) * (len(dims) - 1 - dim))
    return level


def normal_values(own_key, shape, spread, reach, pieces=(), kind=jnp.bfloat16):
    drawn = jax.random.normal(own_key, shape, jnp.float32) * spread
    if len(pieces) > 0:
        drawn = shard_levels(own_key, shape, pieces, -0.22, 0.18) * drawn
    return jnp.clip(drawn, min=-reach, max=reach).astype(kind)


def setup_inputs(seed: int = 0) -> dict:
    key_list = jax.random.split(jax.random.key(seed), 10)
    activations = normal_values(key_list[0], (SECTIONS, MB, SLOTS, FFW), 1.0, 6.0, ((0, 8), (2, 64)))
    out_grads = normal_values(key_list[1], (SECTIONS, MB, SLOTS, D), 1.0, 6.0, ((0, 8), (2, 64)))
    basis_in = normal_values(key_list[2], (SECTIONS, FFW, RANK), FFW ** -0.5, 0.046875, ((0, 8), (1, 64)))
    basis_out = normal_values(key_list[3], (SECTIONS, D, RANK), D ** -0.5, 0.09375, ((0, 8), (1, 64)))
    eigen_values = jnp.clip(jnp.exp(math.log(2.0) - 4.6051702 * jax.random.uniform(key_list[4], (SECTIONS, RANK, RANK), jnp.float32) ** shard_levels(key_list[4], (SECTIONS, RANK, RANK), ((0, 8), (1, 64)), -0.2, 0.2)), 0.02, 2.0)
    query_proj = normal_values(key_list[5], (SECTIONS, QUERIES, RANK, RANK), (RANK * RANK // 64) ** -0.5, 0.046875, ((0, 8), (2, 64)))
    lengths = with_ends(jax.random.randint(key_list[6], (MB,), SLOTS // 4, SLOTS + 1), jax.random.fold_in(key_list[6], 1), SLOTS // 4, SLOTS).astype(jnp.int32)
    seq_rows = with_ends(jax.random.randint(key_list[7], (MB,), 0, TABLE), jax.random.fold_in(key_list[7], 1), 0, TABLE - 1).astype(jnp.int32)
    prior_table = normal_values(key_list[8], (TABLE, QUERIES), 1.0, 6.0, ((0, 64),), jnp.float32)
    return dict(activations=activations, out_grads=out_grads, basis_in=basis_in, basis_out=basis_out, eigen_values=eigen_values, query_proj=query_proj, lengths=lengths, seq_rows=seq_rows, prior_table=prior_table)


DAMPING = 0.01


def reference(activations, out_grads, basis_in, basis_out, eigen_values, query_proj, lengths, seq_rows, prior_table):
    position = jnp.arange(SLOTS, dtype=jnp.int32)
    live_mask = (position[None, :] < lengths[:, None]).reshape(MB * SLOTS, 1)
    inverse_len = 1.0 / lengths.astype(jnp.float32)
    owner_mask = (seq_rows[None, :] == jnp.arange(TABLE, dtype=jnp.int32)[:, None]).astype(jnp.float32)
    running = jnp.zeros((MB, QUERIES), jnp.float32)
    layers_out = []
    for section_index in range(SECTIONS):
        act_proj = jnp.dot(activations[section_index].reshape(MB * SLOTS, FFW), basis_in[section_index], preferred_element_type=jnp.float32).astype(jnp.bfloat16)
        grad_proj = jnp.dot(out_grads[section_index].reshape(MB * SLOTS, D), basis_out[section_index], preferred_element_type=jnp.float32).astype(jnp.bfloat16)
        grad_proj = jnp.where(live_mask, grad_proj, jnp.zeros_like(grad_proj))
        act_proj = lax.optimization_barrier(act_proj)
        grad_proj = lax.optimization_barrier(grad_proj)
        seq_grad = jnp.einsum("mti,mtj->mij", grad_proj.astype(jnp.float32).reshape(MB, SLOTS, RANK), act_proj.astype(jnp.float32).reshape(MB, SLOTS, RANK), precision=lax.Precision.HIGHEST)
        seq_grad = seq_grad * inverse_len[:, None, None]
        precond = (query_proj[section_index].astype(jnp.float32) / (eigen_values[section_index][None] + DAMPING)).astype(jnp.bfloat16)
        precond = lax.optimization_barrier(precond).astype(jnp.float32)
        layer_score = jnp.dot(seq_grad.reshape(MB, RANK * RANK), precond.reshape(QUERIES, RANK * RANK).T, precision=lax.Precision.HIGHEST)
        running = running + layer_score
        layers_out.append(prior_table + jnp.dot(owner_mask, running, precision=lax.Precision.HIGHEST))
    return jnp.stack(layers_out)
```

```python
import functools

import jax
import jax.numpy as jnp
from jax import lax
from jax.experimental import pallas as pl
from jax.experimental.pallas import tpu as pltpu
from jax.sharding import PartitionSpec as P

DAMPING = 0.01
MESH = pl.DeviceIdType.MESH
NX = 4
NC = 2
KA = 224
KG = 64
WIN = 512
HIGH = lax.Precision.HIGHEST


def far_first(n):
    return sorted(range(1, n), key=lambda k: -min(k, n - k))


def kernel(
    n_sections,
    nz,
    a_hbm,
    g_hbm,
    b_hbm,
    w_hbm,
    e_hbm,
    q_hbm,
    len_ref,
    rows_ref,
    prior_ref,
    out_ref,
    a_v,
    g_v,
    e_v,
    q_v,
    b_full,
    w_full,
    w_t,
    p_send,
    p_full,
    x_recv,
    z_send,
    tok,
    xs_a,
    xs_g,
    xr_a,
    xr_g,
    zs_a,
    zs_g,
    zr_a,
    zr_g,
    ap_own,
    gp_own,
    ap_full,
    gp_full,
    rows_x,
    s1_send,
    s1_recv,
    s2_send,
    s2_recv,
    s3_send,
    s3_recv,
    load_sem,
    x_ss,
    x_rs,
    z_ss,
    z_rs,
    c_ss,
    c_rs,
    bw_ss,
    bw_rs,
    p_ss,
    p_rs,
    rx_ss,
    rx_rs,
    rz_ss,
    rz_rs,
    az_ss,
    az_rs,
    gx_ss,
    gx_rs,
    s1_ss,
    s1_rs,
    s2_ss,
    s2_rs,
    s3_ss,
    s3_rs,
):
    sec = lax.axis_index("section")
    dp = lax.axis_index("dp")
    x = dp // (2 * nz)
    z = (dp % (2 * nz)) // 2
    c = dp % 2
    ib = gp_own.shape[0]
    tz = ap_own.shape[0]
    half = w_full.shape[1]
    kx = x_recv.shape[2] - nz * 2 * KG
    kgx = nz * 2 * KG

    def at(xx, zz, cc):
        return (sec, (xx * nz + zz) * 2 + cc)

    def send(src, dst, ss, rs, dev):
        copy = pltpu.make_async_remote_copy(
            src_ref=src, dst_ref=dst, send_sem=ss, recv_sem=rs, device_id=dev, device_id_type=MESH
        )
        copy.start()
        pending.append(copy)

    def arrived(dst, ss, rs):
        pltpu.make_async_remote_copy(
            src_ref=dst,
            dst_ref=dst,
            send_sem=ss,
            recv_sem=rs,
            device_id=(sec, dp),
            device_id_type=MESH,
        ).wait_recv()

    pending = []
    far_x = far_first(NX)
    far_z = far_first(nz)
    far_s = far_first(n_sections)
    group = [(dx, dc) for dx in (2, 1, 3, 0) for dc in (0, 1) if dx or dc]

    off = pl.multiple_of(64 * (z % 2) + KA * c, 32)
    goff = pl.multiple_of(KG * c, 64)
    mine = pl.ds(pl.multiple_of(half * c, 128), half)
    other = pl.ds(pl.multiple_of(half * (1 - c), 128), half)
    a_own = a_hbm.at[:, pl.ds(pl.multiple_of(kx * x, 128), kx)]
    g_own = g_hbm.at[:, pl.ds(pl.multiple_of(kgx * x, 128), kgx)]
    loads = [
        pltpu.make_async_copy(s, d, load_sem.at[i])
        for i, (s, d) in enumerate(
            (
                (a_hbm, a_v),
                (g_hbm, g_v),
                (a_own, x_recv.at[x, :, pl.ds(0, kx)]),
                (g_own, x_recv.at[x, :, pl.ds(kx, kgx)]),
                (e_hbm, e_v),
                (q_hbm, q_v),
                (b_hbm.at[:, mine], b_full.at[pl.ds(off, KA), :]),
                (w_hbm.at[:, mine], w_full.at[pl.ds(goff, KG), :]),
            )
        )
    ]
    for load in loads:
        load.start()

    barrier = pltpu.get_barrier_semaphore()
    partners = [at(x, (z + k) % nz, c) for k in far_z]
    partners += [((sec + k) % n_sections, dp) for k in far_s]
    partners += [at((x + dx) % NX, z, (c + dc) % 2) for dx, dc in group]
    for dev in partners:
        pl.semaphore_signal(barrier, inc=1, device_id=dev, device_id_type=MESH)
    pl.semaphore_wait(barrier, len(partners))

    loads[0].wait()
    loads[1].wait()
    for k in far_x:
        xx = (x + k) % NX
        dev = at(xx, z, c)
        send(
            a_v.at[:, pl.ds(pl.multiple_of(kx * xx, 128), kx)],
            x_recv.at[x, :, pl.ds(0, kx)],
            x_ss.at[0, k],
            x_rs.at[0, k],
            dev,
        )
        send(
            g_v.at[:, pl.ds(pl.multiple_of(kgx * xx, 128), kgx)],
            x_recv.at[x, :, pl.ds(kx, kgx)],
            x_ss.at[1, k],
            x_rs.at[1, k],
            dev,
        )
    twin = at(x, z, 1 - c)
    send(b_hbm.at[:, other], b_full.at[pl.ds(off, KA), :], bw_ss.at[0], bw_rs.at[0], twin)
    send(w_hbm.at[:, other], w_full.at[pl.ds(goff, KG), :], bw_ss.at[1], bw_rs.at[1], twin)

    zero_at = pl.multiple_of((1 - z % 2) * 2 * KA, 64)
    b_full[pl.ds(zero_at, 64), :] = jnp.zeros((64, half), jnp.bfloat16)
    rows_x[...] = jnp.zeros_like(rows_x)
    loads[4].wait()
    loads[5].wait()
    for b in range(2 * NX):
        cols = slice(128 * b, 128 * b + 128)
        den = e_v[:, cols] + DAMPING
        num = q_v[:, :, cols].astype(jnp.float32)
        p_send[b] = (num / den[None]).astype(jnp.bfloat16)
    for i, (dx, dc) in enumerate(group):
        xx, cc = (x + dx) % NX, (c + dc) % 2
        send(
            p_send.at[4 * cc + xx],
            p_full.at[2 * x + c],
            p_ss.at[i],
            p_rs.at[i],
            at(xx, z, cc),
        )
    p_full[2 * x + c] = p_send[4 * c + x]

    loads[2].wait()
    loads[3].wait()
    for k in far_x:
        xx = (x + NX - k) % NX
        arrived(x_recv.at[xx, :, pl.ds(0, kx)], x_ss.at[0, k], x_rs.at[0, k])
        arrived(x_recv.at[xx, :, pl.ds(kx, kgx)], x_ss.at[1, k], x_rs.at[1, k])
    for zz in range(nz):
        start = 896 * (zz // 2) + 384 * (zz % 2)
        z_send[zz, :, 0:WIN] = jnp.concatenate(
            [x_recv[i, :, start : start + WIN] for i in range(NX)], axis=0
        )
        gs = kx + 2 * KG * zz
        z_send[zz, :, WIN : WIN + 2 * KG] = jnp.concatenate(
            [x_recv[i, :, gs : gs + 2 * KG] for i in range(NX)], axis=0
        )
    for k in far_z:
        zz = (z + k) % nz
        send(z_send.at[zz], tok.at[c, z], z_ss.at[k], z_rs.at[k], at(x, zz, c))
    send(z_send.at[z], tok.at[c, z], c_ss.at[0], c_rs.at[0], twin)
    tok[c, z] = z_send[z]

    loads[6].wait()
    loads[7].wait()
    arrived(w_full.at[pl.ds(pl.multiple_of(KG * (1 - c), 64), KG), :], bw_ss.at[1], bw_rs.at[1])
    w_t[...] = w_full[...].astype(jnp.float32).T.astype(jnp.bfloat16)
    off_twin = pl.multiple_of(64 * (z % 2) + KA * (1 - c), 32)
    arrived(b_full.at[pl.ds(off_twin, KA), :], bw_ss.at[0], bw_rs.at[0])

    for k in reversed(far_z):
        zz = (z + nz - k) % nz
        arrived(tok.at[c, zz], z_ss.at[k], z_rs.at[k])
        send(tok.at[c, zz], tok.at[c, zz], c_ss.at[k], c_rs.at[k], twin)
    arrived(tok.at[1 - c, z], c_ss.at[0], c_rs.at[0])
    for k in reversed(far_z):
        zz = (z + nz - k) % nz
        arrived(tok.at[1 - c, zz], c_ss.at[k], c_rs.at[k])

    tokens = 2 * nz * 16
    grads = tok[:, :, :, WIN : WIN + 2 * KG].reshape(tokens, 2 * KG)
    part_g = lax.dot_general(
        w_t[...], grads, (((1,), (1,)), ((), ())), preferred_element_type=jnp.float32
    ).astype(jnp.bfloat16)
    for i in range(NX):
        for zz in range(nz):
            r = (i // 2) * 2 * nz * ib + zz * 2 * ib + (i % 2) * ib
            xs_g[i, zz] = part_g[r : r + ib, :]
    for k in far_x:
        xx = (x + k) % NX
        send(xs_g.at[xx], xr_g.at[x], rx_ss.at[1, k], rx_rs.at[1, k], at(xx, z, c))
    acts = tok[:, :, :, 0:WIN].reshape(tokens, WIN)
    for i in range(NX):
        xs_a[i] = jnp.dot(
            acts, b_full[:, 128 * i : 128 * i + 128], preferred_element_type=jnp.float32
        ).astype(jnp.bfloat16)
    for k in far_x:
        xx = (x + k) % NX
        send(xs_a.at[xx], xr_a.at[x], rx_ss.at[0, k], rx_rs.at[0, k], at(xx, z, c))

    total = xs_g[x].astype(jnp.float32)
    for k in reversed(far_x):
        xx = (x + NX - k) % NX
        arrived(xr_g.at[xx], rx_ss.at[1, k], rx_rs.at[1, k])
        total = total + xr_g[xx].astype(jnp.float32)
    zs_g[...] = total.astype(jnp.bfloat16)
    for k in far_z:
        zz = (z + k) % nz
        send(zs_g.at[zz], zr_g.at[z], rz_ss.at[1, k], rz_rs.at[1, k], at(x, zz, c))
    total = xs_a[x].astype(jnp.float32)
    for k in reversed(far_x):
        xx = (x + NX - k) % NX
        arrived(xr_a.at[xx], rx_ss.at[0, k], rx_rs.at[0, k])
        total = total + xr_a[xx].astype(jnp.float32)
    zs_a[...] = total.astype(jnp.bfloat16).reshape(nz, tz, 128)
    for k in far_z:
        zz = (z + k) % nz
        send(zs_a.at[zz], zr_a.at[z], rz_ss.at[0, k], rz_rs.at[0, k], at(x, zz, c))

    total = zs_g[z].astype(jnp.float32)
    for k in reversed(far_z):
        zz = (z + nz - k) % nz
        arrived(zr_g.at[zz], rz_ss.at[1, k], rz_rs.at[1, k])
        total = total + zr_g[zz].astype(jnp.float32)
    gp_own[...] = total.astype(jnp.bfloat16)
    for i, (dx, dc) in enumerate(group):
        xx, cc = (x + dx) % NX, (c + dc) % 2
        send(gp_own, gp_full.at[4 * c + x], gx_ss.at[i], gx_rs.at[i], at(xx, z, cc))
    gp_full[4 * c + x] = total.astype(jnp.bfloat16)
    total = zs_a[z].astype(jnp.float32)
    for k in reversed(far_z):
        zz = (z + nz - k) % nz
        arrived(zr_a.at[zz], rz_ss.at[0, k], rz_rs.at[0, k])
        total = total + zr_a[zz].astype(jnp.float32)
    ap_own[...] = total.astype(jnp.bfloat16)
    for k in far_z:
        zz = (z + k) % nz
        send(ap_own, ap_full.at[z], az_ss.at[k], az_rs.at[k], at(x, zz, c))
    ap_full[z] = total.astype(jnp.bfloat16)

    for i, (dx, dc) in enumerate(group):
        xx, cc = (x + NX - dx) % NX, (c + 2 - dc) % 2
        arrived(p_full.at[2 * xx + cc], p_ss.at[i], p_rs.at[i])
        arrived(gp_full.at[4 * cc + xx], gx_ss.at[i], gx_rs.at[i])
    for k in reversed(far_z):
        zz = (z + nz - k) % nz
        arrived(ap_full.at[zz], az_ss.at[k], az_rs.at[k])
    lane = lax.broadcasted_iota(jnp.int32, (8 * ib, tokens), 1)
    micro = lane % 4
    slot = ((lane // 4) % 4) * 2 * nz + ((lane // 16) % nz) * 2 + lane // (16 * nz)
    gp = gp_full[...].reshape(8 * ib, tokens).astype(jnp.float32)
    ap = ap_full[...].reshape(tokens, 128)
    for m in range(4):
        live = jnp.where(micro == m, slot, 2**20) < len_ref[m]
        seq = jnp.dot(
            jnp.where(live, gp, 0.0).astype(jnp.bfloat16), ap, preferred_element_type=jnp.float32
        )
        for q in range(8):
            row = seq * p_full[:, q].reshape(8 * ib, 128).astype(jnp.float32)
            rows_x[m * 8 + q : m * 8 + q + 1, :] = jnp.sum(row, axis=0, keepdims=True)
    score = lax.dot_general(
        jnp.ones((8, 128), jnp.float32),
        rows_x[...],
        (((1,), (1,)), ((), ())),
        precision=HIGH,
        preferred_element_type=jnp.float32,
    )
    s1_send[...] = score[0:1, :]
    for i, (dx, dc) in enumerate(group):
        xx, cc = (x + dx) % NX, (c + dc) % 2
        send(s1_send, s1_recv.at[i], s1_ss.at[i], s1_rs.at[i], at(xx, z, cc))
    acc = score[0:1, :]
    for i, (dx, dc) in enumerate(group):
        arrived(s1_recv.at[i], s1_ss.at[i], s1_rs.at[i])
        acc = acc + s1_recv[i]
    s2_send[...] = acc
    for k in far_z:
        send(s2_send, s2_recv.at[k], s2_ss.at[k], s2_rs.at[k], at(x, (z + k) % nz, c))
    for k in reversed(far_z):
        arrived(s2_recv.at[k], s2_ss.at[k], s2_rs.at[k])
        acc = acc + s2_recv[k]
    s3_send[...] = acc
    for k in far_s:
        dev = ((sec + k) % n_sections, dp)
        send(s3_send, s3_recv.at[k], s3_ss.at[k], s3_rs.at[k], dev)
    for k in reversed(far_s):
        arrived(s3_recv.at[k], s3_ss.at[k], s3_rs.at[k])
        acc = acc + jnp.where(sec >= k, s3_recv[k], 0.0)

    lane = lax.broadcasted_iota(jnp.int32, (8, 128), 1)
    row = lax.broadcasted_iota(jnp.int32, (8, 128), 0) + dp * 8
    length = jnp.full((8, 128), 1, jnp.int32)
    target = jnp.full((8, 128), -1, jnp.int32)
    for m in range(4):
        inside = lane // 8 == m
        length = jnp.where(inside, len_ref[m], length)
        target = jnp.where(inside, rows_ref[m], target)
    scaled = acc * (1.0 / length.astype(jnp.float32))
    spread = jnp.where(target == row, scaled, 0.0)
    pick = lax.broadcasted_iota(jnp.int32, (128, 128), 0) % 8
    pick = pick == lax.broadcasted_iota(jnp.int32, (128, 128), 1)
    table = jnp.dot(
        spread, pick.astype(jnp.float32), precision=HIGH, preferred_element_type=jnp.float32
    )
    out_ref[...] = prior_ref[...] + table[:, 0:8]
    for copy in pending:
        copy.wait_send()


def per_device(n_sections, nz, acts, grads, basis_in, basis_out, eig, query, lengths, rows, prior):
    ff, d = acts.shape[3], grads.shape[3]
    rank = basis_in.shape[2]
    half = rank // 2
    ib = eig.shape[1]
    tokens = 2 * nz * 16
    tz = tokens // nz
    kx, kgx = ff // NX, d // NX
    bf, f32 = jnp.bfloat16, jnp.float32
    dma = pltpu.SemaphoreType.DMA
    vm = pltpu.VMEM
    hbm = pl.BlockSpec(memory_space=pl.ANY)
    smem = pl.BlockSpec(memory_space=pltpu.SMEM)
    vmem = pl.BlockSpec(memory_space=pltpu.VMEM)
    out = pl.pallas_call(
        functools.partial(kernel, n_sections, nz),
        out_shape=jax.ShapeDtypeStruct(prior.shape, f32),
        in_specs=[hbm] * 6 + [smem] * 2 + [vmem],
        out_specs=vmem,
        scratch_shapes=[
            vm((4, ff), bf),
            vm((4, d), bf),
            vm((ib, rank), f32),
            vm((8, ib, rank), bf),
            vm((WIN, half), bf),
            vm((2 * KG, half), bf),
            vm((half, 2 * KG), bf),
            vm((2 * NX, 8, ib, 128), bf),
            vm((2 * NX, 8, ib, 128), bf),
            vm((NX, 4, kx + kgx), bf),
            vm((nz, 16, WIN + 2 * KG), bf),
            vm((2, nz, 16, WIN + 2 * KG), bf),
            vm((NX, tokens, 128), bf),
            vm((NX, nz, ib, tokens), bf),
            vm((NX, tokens, 128), bf),
            vm((NX, nz, ib, tokens), bf),
            vm((nz, tz, 128), bf),
            vm((nz, ib, tokens), bf),
            vm((nz, tz, 128), bf),
            vm((nz, ib, tokens), bf),
            vm((tz, 128), bf),
            vm((ib, tokens), bf),
            vm((nz, tz, 128), bf),
            vm((2 * NX, ib, tokens), bf),
            vm((128, 128), f32),
            vm((1, 128), f32),
            vm((2 * NX, 1, 128), f32),
            vm((1, 128), f32),
            vm((nz, 1, 128), f32),
            vm((1, 128), f32),
            vm((n_sections, 1, 128), f32),
            dma((8,)),
            dma((2, NX)),
            dma((2, NX)),
            dma((nz,)),
            dma((nz,)),
            dma((nz,)),
            dma((nz,)),
            dma((2,)),
            dma((2,)),
            dma((7,)),
            dma((7,)),
            dma((2, NX)),
            dma((2, NX)),
            dma((2, nz)),
            dma((2, nz)),
            dma((nz,)),
            dma((nz,)),
            dma((7,)),
            dma((7,)),
            dma((7,)),
            dma((7,)),
            dma((nz,)),
            dma((nz,)),
            dma((n_sections,)),
            dma((n_sections,)),
        ],
        compiler_params=pltpu.CompilerParams(collective_id=0, has_side_effects=True),
    )(
        acts.reshape(4, ff),
        grads.reshape(4, d),
        basis_in[0],
        basis_out[0],
        eig[0],
        query[0],
        lengths,
        rows,
        prior,
    )
    return out[None]


def solution(mesh):
    n_sections, n_dp = mesh.shape["section"], mesh.shape["dp"]
    return jax.shard_map(
        functools.partial(per_device, n_sections, n_dp // (NX * NC)),
        mesh=mesh,
        in_specs=(
            P("section", None, "dp", None),
            P("section", None, "dp", None),
            P("section", "dp", None),
            P("section", "dp", None),
            P("section", "dp", None),
            P("section", None, "dp", None),
            P(),
            P(),
            P("dp", None),
        ),
        out_specs=P("section", "dp", None),
        check_vma=False,
    )
```

```python
import functools

import jax
import jax.numpy as jnp
from jax import lax
from jax.experimental import pallas as pl
from jax.experimental.pallas import tpu as pltpu
from jax.sharding import PartitionSpec as P

DAMPING = 0.01
MESH = pl.DeviceIdType.MESH
NX = 4
NC = 2
KA = 224
KG = 64
WIN = 512
SEMS = ("x", "z", "c", "bw", "p", "rx", "rz", "az", "gx", "s1", "s2", "s3")
HIGH = lax.Precision.HIGHEST


def far_first(n):
    return sorted(range(1, n), key=lambda k: -min(k, n - k))


def kernel(
    n_sections,
    nz,
    a_hbm,
    g_hbm,
    b_hbm,
    w_hbm,
    e_hbm,
    q_hbm,
    len_hbm,
    rows_hbm,
    prior_hbm,
    out_ref,
    len_ref,
    rows_ref,
    prior_ref,
    a_v,
    g_v,
    e_v,
    q_v,
    b_full,
    w_full,
    w_t,
    p_send,
    p_full,
    x_recv,
    z_send_a,
    z_send_g,
    tok_a,
    tok_g,
    xs_a,
    xs_g,
    xr_a,
    xr_g,
    zs_a,
    zs_g,
    zr_a,
    zr_g,
    ap_own,
    gp_own,
    ap_full,
    gp_full,
    rows_x,
    s1_send,
    s1_recv,
    s2_send,
    s2_recv,
    s3_send,
    s3_recv,
    load_sem,
    ready,
    *sem_refs,
):
    sec = lax.axis_index("section")
    dp = lax.axis_index("dp")
    x = dp // (2 * nz)
    z = (dp % (2 * nz)) // 2
    c = dp % 2
    ib = gp_own.shape[0]
    tz = ap_own.shape[0]
    half = w_full.shape[1]
    kgx = nz * 2 * KG
    kx = x_recv.shape[2] - kgx
    sems = dict(zip(SEMS, sem_refs, strict=True))

    def at(xx, zz, cc):
        return (sec, (xx * nz + zz) * 2 + cc)

    def copy_of(src, dst, name, i, dev):
        return pltpu.make_async_remote_copy(
            src_ref=src,
            dst_ref=dst,
            send_sem=sems[name].at[(0, *i)],
            recv_sem=sems[name].at[(1, *i)],
            device_id=dev,
            device_id_type=MESH,
        )

    def send(src, dst, name, i, dev):
        copy = copy_of(src, dst, name, i, dev)
        copy.start()
        pending.append(copy)

    def arrived(dst, name, i):
        copy_of(dst, dst, name, i, (sec, dp)).wait_recv()

    pending = []
    far_x = far_first(NX)
    far_z = far_first(nz)
    near_z = far_z[::-1]
    far_s = far_first(n_sections)
    group = [(dx, dc) for dx in (2, 1, 3, 0) for dc in (0, 1) if dx or dc]

    barrier = pltpu.get_barrier_semaphore()
    partners = [at((x + dx) % NX, z, (c + dc) % 2) for dx, dc in group]
    partners += [at(x, (z + k) % nz, c) for k in far_z]
    for dev in partners:
        pl.semaphore_signal(barrier, inc=1, device_id=dev, device_id_type=MESH)
    for k in far_s:

        @pl.when(sec + k < n_sections)
        def _(k=k):
            pl.semaphore_signal(barrier, inc=1, device_id=(sec + k, dp), device_id_type=MESH)

    off = pl.multiple_of(64 * (z % 2) + KA * c, 32)
    off_twin = pl.multiple_of(64 * (z % 2) + KA * (1 - c), 32)
    goff = pl.multiple_of(KG * c, 64)
    goff_twin = pl.multiple_of(KG * (1 - c), 64)
    mine = pl.ds(pl.multiple_of(half * c, 128), half)
    other = pl.ds(pl.multiple_of(half * (1 - c), 128), half)
    a_own = a_hbm.at[:, pl.ds(pl.multiple_of(kx * x, 128), kx)]
    g_own = g_hbm.at[:, pl.ds(pl.multiple_of(kgx * x, 128), kgx)]
    loads = [
        pltpu.make_async_copy(s, d, load_sem.at[i])
        for i, (s, d) in enumerate(
            (
                (g_hbm, g_v),
                (a_hbm, a_v),
                (g_own, x_recv.at[x, :, pl.ds(kx, kgx)]),
                (a_own, x_recv.at[x, :, pl.ds(0, kx)]),
                (e_hbm, e_v),
                (q_hbm, q_v),
                (b_hbm.at[:, mine], b_full.at[pl.ds(off, KA), :]),
                (w_hbm.at[:, mine], w_full.at[pl.ds(goff, KG), :]),
                (len_hbm, len_ref),
                (rows_hbm, rows_ref),
                (prior_hbm, prior_ref),
            )
        )
    ]
    for load in loads:
        load.start()

    pl.semaphore_wait(barrier, len(partners) + sec)

    loads[0].wait()
    for k in far_x:
        xx = (x + k) % NX
        send(
            g_v.at[:, pl.ds(pl.multiple_of(kgx * xx, 128), kgx)],
            x_recv.at[x, :, pl.ds(kx, kgx)],
            "x",
            (1, k),
            at(xx, z, c),
        )
    loads[1].wait()
    for k in far_x:
        xx = (x + k) % NX
        send(
            a_v.at[:, pl.ds(pl.multiple_of(kx * xx, 128), kx)],
            x_recv.at[x, :, pl.ds(0, kx)],
            "x",
            (0, k),
            at(xx, z, c),
        )
    twin = at(x, z, 1 - c)
    send(b_hbm.at[:, other], b_full.at[pl.ds(off, KA), :], "bw", (0,), twin)
    send(w_hbm.at[:, other], w_full.at[pl.ds(goff, KG), :], "bw", (1,), twin)

    zero_at = pl.multiple_of((1 - z % 2) * 2 * KA, 64)
    b_full[pl.ds(zero_at, 64), :] = jnp.zeros((64, half), jnp.bfloat16)
    rows_x[...] = jnp.zeros_like(rows_x)
    loads[4].wait()
    loads[5].wait()
    for b in range(2 * NX):
        cols = slice(128 * b, 128 * b + 128)
        den = e_v[:, cols] + DAMPING
        num = q_v[:, :, cols].astype(jnp.float32)
        p_send[b] = (num / den[None]).astype(jnp.bfloat16)
    p_full[2 * x + c] = p_send[4 * c + x]

    loads[2].wait()
    for k in far_x:
        arrived(x_recv.at[(x + NX - k) % NX, :, pl.ds(kx, kgx)], "x", (1, k))
    for zz in range(nz):
        gs = kx + 2 * KG * zz
        z_send_g[zz] = jnp.concatenate(
            [x_recv[i, :, gs : gs + 2 * KG] for i in range(NX)], axis=0
        )
    for k in far_z:
        zz = (z + k) % nz
        send(z_send_g.at[zz], tok_g.at[z, c], "z", (1, k), at(x, zz, c))
    send(z_send_g.at[z], tok_g.at[z, c], "c", (1, 0), twin)
    tok_g[z, c] = z_send_g[z]
    loads[3].wait()
    for k in far_x:
        arrived(x_recv.at[(x + NX - k) % NX, :, pl.ds(0, kx)], "x", (0, k))
    for zz in range(nz):
        start = 896 * (zz // 2) + 384 * (zz % 2)
        z_send_a[zz] = jnp.concatenate(
            [x_recv[i, :, start : start + WIN] for i in range(NX)], axis=0
        )
    for k in far_z:
        zz = (z + k) % nz
        send(z_send_a.at[zz], tok_a.at[z, c], "z", (0, k), at(x, zz, c))
    send(z_send_a.at[z], tok_a.at[z, c], "c", (0, 0), twin)
    tok_a[z, c] = z_send_a[z]

    for k in far_s:

        @pl.when(sec >= k)
        def _(k=k):
            pl.semaphore_signal(ready, inc=1, device_id=(sec - k, dp), device_id_type=MESH)

    loads[6].wait()
    loads[7].wait()
    arrived(w_full.at[pl.ds(goff_twin, KG), :], "bw", (1,))
    w_t[...] = w_full[...].astype(jnp.float32).T.astype(jnp.bfloat16)
    arrived(b_full.at[pl.ds(off_twin, KA), :], "bw", (0,))

    tokens = nz * tz

    def forward(tok, kind, k):
        zz = (z + nz - k) % nz
        arrived(tok.at[zz, c], "z", (kind, k))
        send(tok.at[zz, c], tok.at[zz, c], "c", (kind, k), twin)

    def project_acts(k):
        zz = (z + nz - k) % nz
        arrived(tok_a.at[zz, 1 - c], "c", (0, k))
        part = jnp.dot(
            tok_a[zz].reshape(tz, WIN), b_full[...], preferred_element_type=jnp.float32
        ).astype(jnp.bfloat16)
        for i in range(NX):
            xs_a[zz, i] = part[:, 128 * i : 128 * i + 128]
        for kx_ in far_x:
            xx = (x + kx_) % NX
            send(xs_a.at[zz, xx], xr_a.at[zz, x], "rx", (0, k, kx_), at(xx, z, c))

    def project_grads():
        for k in near_z:
            forward(tok_g, 1, k)
        for k in [0] + near_z:
            arrived(tok_g.at[(z + nz - k) % nz, 1 - c], "c", (1, k))
        part = lax.dot_general(
            w_t[...],
            tok_g[...].reshape(tokens, 2 * KG),
            (((1,), (1,)), ((), ())),
            preferred_element_type=jnp.float32,
        ).astype(jnp.bfloat16)
        for i in range(NX):
            for zz in range(nz):
                r = (i // 2) * 2 * nz * ib + zz * 2 * ib + (i % 2) * ib
                xs_g[zz, i] = part[r : r + ib, :]
        for k in far_z + [0]:
            zz = (z + k) % nz
            for kx_ in far_x:
                xx = (x + kx_) % NX
                send(xs_g.at[zz, xx], xr_g.at[zz, x], "rx", (1, k, kx_), at(xx, z, c))

    def sum_over_x(sent, recv, out, kind, k, zz):
        total = sent[zz, x].astype(jnp.float32)
        for kx_ in far_x:
            xx = (x + NX - kx_) % NX
            arrived(recv.at[zz, xx], "rx", (kind, k, kx_))
            total = total + recv[zz, xx].astype(jnp.float32)
        out[zz] = total.astype(jnp.bfloat16)

    def sum_over_z(sums, recv, kind):
        total = sums[z].astype(jnp.float32)
        for k in near_z:
            zz = (z + nz - k) % nz
            arrived(recv.at[zz], "rz", (kind, k))
            total = total + recv[zz].astype(jnp.float32)
        return total.astype(jnp.bfloat16)

    order = [0] + near_z
    split = min(3, nz - 1)
    for i, k in enumerate(order):
        if i == split:
            project_grads()
        if k:
            forward(tok_a, 0, k)
        if i:
            project_acts(order[i - 1])
    project_acts(order[-1])
    for i, (dx, dc) in enumerate(group):
        xx, cc = (x + dx) % NX, (c + dc) % 2
        send(p_send.at[4 * cc + xx], p_full.at[2 * x + c], "p", (i,), at(xx, z, cc))

    for k in far_z + [0]:
        zz = (z + k) % nz
        sum_over_x(xs_g, xr_g, zs_g, 1, k, zz)
        if k:
            send(zs_g.at[zz], zr_g.at[z], "rz", (1, k), at(x, zz, c))
    for k in order:
        zz = (z + nz - k) % nz
        sum_over_x(xs_a, xr_a, zs_a, 0, k, zz)
        if k:
            send(zs_a.at[zz], zr_a.at[z], "rz", (0, nz - k), at(x, zz, c))
    own = sum_over_z(zs_g, zr_g, 1)
    gp_own[...] = own
    for i, (dx, dc) in enumerate(group):
        xx, cc = (x + dx) % NX, (c + dc) % 2
        send(gp_own, gp_full.at[4 * c + x], "gx", (i,), at(xx, z, cc))
    gp_full[4 * c + x] = own
    own = sum_over_z(zs_a, zr_a, 0)
    ap_own[...] = own
    for k in far_z:
        send(ap_own, ap_full.at[z], "az", (k,), at(x, (z + k) % nz, c))
    ap_full[z] = own

    for i, (dx, dc) in enumerate(group):
        xx, cc = (x + NX - dx) % NX, (c + 2 - dc) % 2
        arrived(p_full.at[2 * xx + cc], "p", (i,))
        arrived(gp_full.at[4 * cc + xx], "gx", (i,))
    for k in near_z:
        arrived(ap_full.at[(z + nz - k) % nz], "az", (k,))
    for load in loads[8:]:
        load.wait()
    lane = lax.broadcasted_iota(jnp.int32, (8 * ib, tokens), 1)
    micro = lane % 4
    slot = ((lane // 4) % 4) * 2 * nz + (lane // tz) * 2 + (lane // 16) % 2
    gp = gp_full[...].reshape(8 * ib, tokens).astype(jnp.float32)
    ap = ap_full[...].reshape(tokens, 128)
    for m in range(4):
        live = jnp.where(micro == m, slot, 2**20) < len_ref[m]
        seq = jnp.dot(
            jnp.where(live, gp, 0.0).astype(jnp.bfloat16), ap, preferred_element_type=jnp.float32
        )
        for q in range(8):
            row = seq * p_full[:, q].reshape(8 * ib, 128).astype(jnp.float32)
            rows_x[m * 8 + q : m * 8 + q + 1, :] = jnp.sum(row, axis=0, keepdims=True)
    score = lax.dot_general(
        jnp.ones((8, 128), jnp.float32),
        rows_x[...],
        (((1,), (1,)), ((), ())),
        precision=HIGH,
        preferred_element_type=jnp.float32,
    )
    s1_send[...] = score[0:1, :]
    for i, (dx, dc) in enumerate(group):
        xx, cc = (x + dx) % NX, (c + dc) % 2
        send(s1_send, s1_recv.at[i], "s1", (i,), at(xx, z, cc))
    acc = score[0:1, :]
    for i in range(len(group)):
        arrived(s1_recv.at[i], "s1", (i,))
        acc = acc + s1_recv[i]
    s2_send[...] = acc
    for k in far_z:
        send(s2_send, s2_recv.at[k], "s2", (k,), at(x, (z + k) % nz, c))
    for k in near_z:
        arrived(s2_recv.at[k], "s2", (k,))
        acc = acc + s2_recv[k]
    s3_send[...] = acc

    def score_copy(k):
        return copy_of(s3_send, s3_recv.at[k], "s3", (k,), ((sec + k) % n_sections, dp))


    @pl.when(sec < n_sections - 1)
    def _():
        pl.semaphore_wait(ready, n_sections - 1 - sec)

    for k in far_s:

        @pl.when(sec + k < n_sections)
        def _(k=k):
            score_copy(k).start()

    for k in reversed(far_s):

        @pl.when(sec >= k)
        def _(k=k):
            score_copy(k).wait_recv()

        acc = acc + jnp.where(sec >= k, s3_recv[k], 0.0)

    lane = lax.broadcasted_iota(jnp.int32, (8, 128), 1)
    row = lax.broadcasted_iota(jnp.int32, (8, 128), 0) + dp * 8
    length = jnp.full((8, 128), 1, jnp.int32)
    target = jnp.full((8, 128), -1, jnp.int32)
    for m in range(4):
        inside = lane // 8 == m
        length = jnp.where(inside, len_ref[m], length)
        target = jnp.where(inside, rows_ref[m], target)
    scaled = acc * (1.0 / length.astype(jnp.float32))
    spread = jnp.where(target == row, scaled, 0.0)
    pick = lax.broadcasted_iota(jnp.int32, (128, 128), 0) % 8
    pick = pick == lax.broadcasted_iota(jnp.int32, (128, 128), 1)
    table = jnp.dot(
        spread, pick.astype(jnp.float32), precision=HIGH, preferred_element_type=jnp.float32
    )
    out_ref[...] = prior_ref[...] + table[:, 0:8]
    for copy in pending:
        copy.wait_send()
    for k in far_s:

        @pl.when(sec + k < n_sections)
        def _(k=k):
            score_copy(k).wait_send()


def per_device(n_sections, nz, acts, grads, basis_in, basis_out, eig, query, lengths, rows, prior):
    ff, d = acts.shape[3], grads.shape[3]
    rank = basis_in.shape[2]
    half = rank // 2
    ib = eig.shape[1]
    tokens = 2 * nz * 16
    tz = tokens // nz
    kx, kgx = ff // NX, d // NX
    bf, f32 = jnp.bfloat16, jnp.float32
    dma = pltpu.SemaphoreType.DMA
    vm = pltpu.VMEM
    hbm = pl.BlockSpec(memory_space=pl.ANY)
    vmem = pl.BlockSpec(memory_space=pltpu.VMEM)
    out = pl.pallas_call(
        functools.partial(kernel, n_sections, nz),
        out_shape=jax.ShapeDtypeStruct(prior.shape, f32),
        in_specs=[hbm] * 9,
        out_specs=vmem,
        scratch_shapes=[
            pltpu.SMEM((4,), jnp.int32),
            pltpu.SMEM((4,), jnp.int32),
            vm(prior.shape, f32),
            vm((4, ff), bf),
            vm((4, d), bf),
            vm((ib, rank), f32),
            vm((8, ib, rank), bf),
            vm((WIN, half), bf),
            vm((2 * KG, half), bf),
            vm((half, 2 * KG), bf),
            vm((2 * NX, 8, ib, 128), bf),
            vm((2 * NX, 8, ib, 128), bf),
            vm((NX, 4, kx + kgx), bf),
            vm((nz, 16, WIN), bf),
            vm((nz, 16, 2 * KG), bf),
            vm((nz, 2, 16, WIN), bf),
            vm((nz, 2, 16, 2 * KG), bf),
            vm((nz, NX, tz, 128), bf),
            vm((nz, NX, ib, tokens), bf),
            vm((nz, NX, tz, 128), bf),
            vm((nz, NX, ib, tokens), bf),
            vm((nz, tz, 128), bf),
            vm((nz, ib, tokens), bf),
            vm((nz, tz, 128), bf),
            vm((nz, ib, tokens), bf),
            vm((tz, 128), bf),
            vm((ib, tokens), bf),
            vm((nz, tz, 128), bf),
            vm((2 * NX, ib, tokens), bf),
            vm((128, 128), f32),
            vm((1, 128), f32),
            vm((2 * NX, 1, 128), f32),
            vm((1, 128), f32),
            vm((nz, 1, 128), f32),
            vm((1, 128), f32),
            vm((n_sections, 1, 128), f32),
            dma((11,)),
            pltpu.SemaphoreType.REGULAR,
            dma((2, 2, NX)),
            dma((2, 2, nz)),
            dma((2, 2, nz)),
            dma((2, 2)),
            dma((2, 7)),
            dma((2, 2, nz, NX)),
            dma((2, 2, nz)),
            dma((2, nz)),
            dma((2, 7)),
            dma((2, 7)),
            dma((2, nz)),
            dma((2, n_sections)),
        ],
        compiler_params=pltpu.CompilerParams(collective_id=0, has_side_effects=True),
    )(
        acts.reshape(4, ff),
        grads.reshape(4, d),
        basis_in[0],
        basis_out[0],
        eig[0],
        query[0],
        lengths,
        rows,
        prior,
    )
    return out[None]


def solution(mesh):
    n_sections, n_dp = mesh.shape["section"], mesh.shape["dp"]
    return jax.shard_map(
        functools.partial(per_device, n_sections, n_dp // (NX * NC)),
        mesh=mesh,
        in_specs=(
            P("section", None, "dp", None),
            P("section", None, "dp", None),
            P("section", "dp", None),
            P("section", "dp", None),
            P("section", "dp", None),
            P("section", None, "dp", None),
            P(),
            P(),
            P("dp", None),
        ),
        out_specs=P("section", "dp", None),
        check_vma=False,
    )
```

```python
import functools

import jax
import jax.numpy as jnp
from jax import lax
from jax.experimental import pallas as pl
from jax.experimental.pallas import tpu as pltpu
from jax.sharding import PartitionSpec as P

DAMPING = 0.01
MESH = pl.DeviceIdType.MESH
NX = 4
NC = 2
KA = 224
KG = 64
WIN = 512
SEMS = ("x", "z", "c", "bw", "p", "hx", "rx", "rz", "az", "gx", "s1", "s2", "s3")
HIGH = lax.Precision.HIGHEST


def far_first(n):
    return sorted(range(1, n), key=lambda k: -min(k, n - k))


def kernel(
    n_sections,
    nz,
    a_hbm,
    g_hbm,
    b_hbm,
    w_hbm,
    e_hbm,
    q_hbm,
    len_hbm,
    rows_hbm,
    prior_hbm,
    out_ref,
    len_ref,
    rows_ref,
    prior_ref,
    a_v,
    g_v,
    e_v,
    q_v,
    b_full,
    w_full,
    w_t,
    p_send,
    p_full,
    x_recv,
    z_send_a,
    z_send_g,
    tok_a,
    tok_g,
    xs_a,
    xs_g,
    xh_a,
    xh_g,
    xr_a,
    xr_g,
    zs_a,
    zs_g,
    zr_a,
    zr_g,
    ap_own,
    gp_own,
    ap_full,
    gp_full,
    rows_x,
    s1_send,
    s1_recv,
    s2_send,
    s2_recv,
    s3_send,
    s3_recv,
    load_sem,
    ready,
    *sem_refs,
):
    sec = lax.axis_index("section")
    dp = lax.axis_index("dp")
    x = dp // (2 * nz)
    z = (dp % (2 * nz)) // 2
    c = dp % 2
    ib = gp_own.shape[0]
    tz = ap_own.shape[0]
    half = w_full.shape[1]
    kgx = nz * 2 * KG
    kx = x_recv.shape[2] - kgx
    sems = dict(zip(SEMS, sem_refs, strict=True))

    def at(xx, zz, cc):
        return (sec, (xx * nz + zz) * 2 + cc)

    def copy_of(src, dst, name, i, dev):
        return pltpu.make_async_remote_copy(
            src_ref=src,
            dst_ref=dst,
            send_sem=sems[name].at[(0, *i)],
            recv_sem=sems[name].at[(1, *i)],
            device_id=dev,
            device_id_type=MESH,
        )

    def send(src, dst, name, i, dev):
        copy = copy_of(src, dst, name, i, dev)
        copy.start()
        pending.append(copy)

    def arrived(dst, name, i):
        copy_of(dst, dst, name, i, (sec, dp)).wait_recv()

    pending = []
    far_x = far_first(NX)
    far_z = far_first(nz)
    near_z = far_z[::-1]
    far_s = far_first(n_sections)
    group = [(dx, dc) for dx in (2, 1, 3, 0) for dc in (0, 1) if dx or dc]

    barrier = pltpu.get_barrier_semaphore()
    partners = [at((x + dx) % NX, z, (c + dc) % 2) for dx, dc in group]
    partners += [at(x, (z + k) % nz, c) for k in far_z]
    for dev in partners:
        pl.semaphore_signal(barrier, inc=1, device_id=dev, device_id_type=MESH)
    for k in far_s:

        @pl.when(sec + k < n_sections)
        def _(k=k):
            pl.semaphore_signal(barrier, inc=1, device_id=(sec + k, dp), device_id_type=MESH)

    off = pl.multiple_of(64 * (z % 2) + KA * c, 32)
    off_twin = pl.multiple_of(64 * (z % 2) + KA * (1 - c), 32)
    goff = pl.multiple_of(KG * c, 64)
    goff_twin = pl.multiple_of(KG * (1 - c), 64)
    mine = pl.ds(pl.multiple_of(half * c, 128), half)
    other = pl.ds(pl.multiple_of(half * (1 - c), 128), half)
    a_own = a_hbm.at[:, pl.ds(pl.multiple_of(kx * x, 128), kx)]
    g_own = g_hbm.at[:, pl.ds(pl.multiple_of(kgx * x, 128), kgx)]
    loads = [
        pltpu.make_async_copy(s, d, load_sem.at[i])
        for i, (s, d) in enumerate(
            (
                (g_hbm, g_v),
                (a_hbm, a_v),
                (g_own, x_recv.at[x, :, pl.ds(kx, kgx)]),
                (a_own, x_recv.at[x, :, pl.ds(0, kx)]),
                (e_hbm, e_v),
                (q_hbm, q_v),
                (b_hbm.at[:, mine], b_full.at[pl.ds(off, KA), :]),
                (w_hbm.at[:, mine], w_full.at[pl.ds(goff, KG), :]),
                (len_hbm, len_ref),
                (rows_hbm, rows_ref),
                (prior_hbm, prior_ref),
            )
        )
    ]
    for load in loads:
        load.start()

    pl.semaphore_wait(barrier, len(partners) + sec)

    loads[0].wait()
    for k in far_x:
        xx = (x + k) % NX
        send(
            g_v.at[:, pl.ds(pl.multiple_of(kgx * xx, 128), kgx)],
            x_recv.at[x, :, pl.ds(kx, kgx)],
            "x",
            (1, k),
            at(xx, z, c),
        )
    loads[1].wait()
    for k in far_x:
        xx = (x + k) % NX
        send(
            a_v.at[:, pl.ds(pl.multiple_of(kx * xx, 128), kx)],
            x_recv.at[x, :, pl.ds(0, kx)],
            "x",
            (0, k),
            at(xx, z, c),
        )
    twin = at(x, z, 1 - c)
    send(b_hbm.at[:, other], b_full.at[pl.ds(off, KA), :], "bw", (0,), twin)
    send(w_hbm.at[:, other], w_full.at[pl.ds(goff, KG), :], "bw", (1,), twin)

    zero_at = pl.multiple_of((1 - z % 2) * 2 * KA, 64)
    b_full[pl.ds(zero_at, 64), :] = jnp.zeros((64, half), jnp.bfloat16)
    rows_x[...] = jnp.zeros_like(rows_x)
    loads[4].wait()
    loads[5].wait()
    for b in range(2 * NX):
        cols = slice(128 * b, 128 * b + 128)
        den = e_v[:, cols] + DAMPING
        num = q_v[:, :, cols].astype(jnp.float32)
        p_send[b] = (num / den[None]).astype(jnp.bfloat16)
    p_full[2 * x + c] = p_send[4 * c + x]

    loads[2].wait()
    for k in far_x:
        arrived(x_recv.at[(x + NX - k) % NX, :, pl.ds(kx, kgx)], "x", (1, k))
    for zz in range(nz):
        gs = kx + 2 * KG * zz
        z_send_g[zz] = jnp.concatenate(
            [x_recv[i, :, gs : gs + 2 * KG] for i in range(NX)], axis=0
        )
    for k in far_z:
        zz = (z + k) % nz
        send(z_send_g.at[zz], tok_g.at[z, c], "z", (1, k), at(x, zz, c))
    send(z_send_g.at[z], tok_g.at[z, c], "c", (1, 0), twin)
    tok_g[z, c] = z_send_g[z]
    loads[3].wait()
    for k in far_x:
        arrived(x_recv.at[(x + NX - k) % NX, :, pl.ds(0, kx)], "x", (0, k))
    for zz in range(nz):
        start = 896 * (zz // 2) + 384 * (zz % 2)
        z_send_a[zz] = jnp.concatenate(
            [x_recv[i, :, start : start + WIN] for i in range(NX)], axis=0
        )
    for k in far_z:
        zz = (z + k) % nz
        send(z_send_a.at[zz], tok_a.at[z, c], "z", (0, k), at(x, zz, c))
    send(z_send_a.at[z], tok_a.at[z, c], "c", (0, 0), twin)
    tok_a[z, c] = z_send_a[z]

    for k in far_s:

        @pl.when(sec >= k)
        def _(k=k):
            pl.semaphore_signal(ready, inc=1, device_id=(sec - k, dp), device_id_type=MESH)

    loads[6].wait()
    loads[7].wait()
    arrived(w_full.at[pl.ds(goff_twin, KG), :], "bw", (1,))
    w_t[...] = w_full[...].astype(jnp.float32).T.astype(jnp.bfloat16)
    arrived(b_full.at[pl.ds(off_twin, KA), :], "bw", (0,))

    tokens = nz * tz

    def forward(tok, kind, k):
        zz = (z + nz - k) % nz
        arrived(tok.at[zz, c], "z", (kind, k))
        send(tok.at[zz, c], tok.at[zz, c], "c", (kind, k), twin)

    def project_acts(k):
        zz = (z + nz - k) % nz
        arrived(tok_a.at[zz, 1 - c], "c", (0, k))
        part = jnp.dot(
            tok_a[zz].reshape(tz, WIN), b_full[...], preferred_element_type=jnp.float32
        ).astype(jnp.bfloat16)
        for i in range(NX):
            xs_a[zz, i] = part[:, 128 * i : 128 * i + 128]
        h = tz // 2
        send(xs_a.at[zz, facing, 0:h], xh_a.at[zz, 0], "hx", (0, k, 0), at(right, z, c))
        send(xs_a.at[zz, facing, h:tz], xh_a.at[zz, 1], "hx", (0, k, 1), at(left, z, c))

    def relay_acts(k):
        zz = (z + nz - k) % nz
        h = tz // 2
        for side, xx, rows in ((0, right, slice(0, h)), (1, left, slice(h, tz))):
            arrived(xh_a.at[zz, side], "hx", (0, k, side))
            both = xs_a[zz, xx, rows].astype(jnp.float32) + xh_a[zz, side].astype(jnp.float32)
            xs_a[zz, xx, rows] = both.astype(jnp.bfloat16)
            send(xs_a.at[zz, xx], xr_a.at[zz, side], "rx", (0, k, side), at(xx, z, c))

    def project_grads():
        for k in near_z:
            forward(tok_g, 1, k)
        for k in [0] + near_z:
            arrived(tok_g.at[(z + nz - k) % nz, 1 - c], "c", (1, k))
        part = lax.dot_general(
            w_t[...],
            tok_g[...].reshape(tokens, 2 * KG),
            (((1,), (1,)), ((), ())),
            preferred_element_type=jnp.float32,
        ).astype(jnp.bfloat16)
        for i in range(NX):
            for zz in range(nz):
                r = (i // 2) * 2 * nz * ib + zz * 2 * ib + (i % 2) * ib
                xs_g[i, zz] = part[r : r + ib, :]
        h = nz // 2
        send(xs_g.at[facing, 0:h], xh_g.at[0], "hx", (1, 0, 0), at(right, z, c))
        send(xs_g.at[facing, h:nz], xh_g.at[1], "hx", (1, 0, 1), at(left, z, c))

    def relay_grads():
        h = nz // 2
        for side, xx, rows in ((0, right, slice(0, h)), (1, left, slice(h, nz))):
            arrived(xh_g.at[side], "hx", (1, 0, side))
            both = xs_g[xx, rows].astype(jnp.float32) + xh_g[side].astype(jnp.float32)
            xs_g[xx, rows] = both.astype(jnp.bfloat16)
            send(xs_g.at[xx], xr_g.at[side], "rx", (1, 0, side), at(xx, z, c))

    def sum_over_z(sums, recv, kind):
        total = sums[z].astype(jnp.float32)
        for k in near_z:
            zz = (z + nz - k) % nz
            arrived(recv.at[zz], "rz", (kind, k))
            total = total + recv[zz].astype(jnp.float32)
        return total.astype(jnp.bfloat16)

    right, facing, left = (x + 1) % NX, (x + 2) % NX, (x + 3) % NX
    order = [0] + near_z
    split = min(3, nz - 1)
    for i, k in enumerate(order):
        if i == split:
            project_grads()
        if k:
            forward(tok_a, 0, k)
        if i:
            project_acts(order[i - 1])
        if i >= 4:
            relay_acts(order[i - 4])
    project_acts(order[-1])
    relay_grads()
    for k in order[max(nz - 4, 0) :]:
        relay_acts(k)
    for i, (dx, dc) in enumerate(group):
        xx, cc = (x + dx) % NX, (c + dc) % 2
        send(p_send.at[4 * cc + xx], p_full.at[2 * x + c], "p", (i,), at(xx, z, cc))

    total = xs_g[x].astype(jnp.float32)
    for side in (0, 1):
        arrived(xr_g.at[side], "rx", (1, 0, side))
        total = total + xr_g[side].astype(jnp.float32)
    zs_g[...] = total.astype(jnp.bfloat16)
    for k in far_z:
        zz = (z + k) % nz
        send(zs_g.at[zz], zr_g.at[z], "rz", (1, k), at(x, zz, c))
    for k in order:
        zz = (z + nz - k) % nz
        total = xs_a[zz, x].astype(jnp.float32)
        for side in (0, 1):
            arrived(xr_a.at[zz, side], "rx", (0, k, side))
            total = total + xr_a[zz, side].astype(jnp.float32)
        zs_a[zz] = total.astype(jnp.bfloat16)
        if k:
            send(zs_a.at[zz], zr_a.at[z], "rz", (0, nz - k), at(x, zz, c))
    own = sum_over_z(zs_g, zr_g, 1)
    gp_own[...] = own
    for i, (dx, dc) in enumerate(group):
        xx, cc = (x + dx) % NX, (c + dc) % 2
        send(gp_own, gp_full.at[4 * c + x], "gx", (i,), at(xx, z, cc))
    gp_full[4 * c + x] = own
    own = sum_over_z(zs_a, zr_a, 0)
    ap_own[...] = own
    for k in far_z:
        send(ap_own, ap_full.at[z], "az", (k,), at(x, (z + k) % nz, c))
    ap_full[z] = own

    for i, (dx, dc) in enumerate(group):
        xx, cc = (x + NX - dx) % NX, (c + 2 - dc) % 2
        arrived(p_full.at[2 * xx + cc], "p", (i,))
        arrived(gp_full.at[4 * cc + xx], "gx", (i,))
    for k in near_z:
        arrived(ap_full.at[(z + nz - k) % nz], "az", (k,))
    for load in loads[8:]:
        load.wait()
    lane = lax.broadcasted_iota(jnp.int32, (8 * ib, tokens), 1)
    micro = lane % 4
    slot = ((lane // 4) % 4) * 2 * nz + (lane // tz) * 2 + (lane // 16) % 2
    gp = gp_full[...].reshape(8 * ib, tokens).astype(jnp.float32)
    ap = ap_full[...].reshape(tokens, 128)
    for m in range(4):
        live = jnp.where(micro == m, slot, 2**20) < len_ref[m]
        seq = jnp.dot(
            jnp.where(live, gp, 0.0).astype(jnp.bfloat16), ap, preferred_element_type=jnp.float32
        )
        for q in range(8):
            row = seq * p_full[:, q].reshape(8 * ib, 128).astype(jnp.float32)
            rows_x[m * 8 + q : m * 8 + q + 1, :] = jnp.sum(row, axis=0, keepdims=True)
    score = lax.dot_general(
        jnp.ones((8, 128), jnp.float32),
        rows_x[...],
        (((1,), (1,)), ((), ())),
        precision=HIGH,
        preferred_element_type=jnp.float32,
    )
    s1_send[...] = score[0:1, :]
    for i, (dx, dc) in enumerate(group):
        xx, cc = (x + dx) % NX, (c + dc) % 2
        send(s1_send, s1_recv.at[i], "s1", (i,), at(xx, z, cc))
    acc = score[0:1, :]
    for i in range(len(group)):
        arrived(s1_recv.at[i], "s1", (i,))
        acc = acc + s1_recv[i]
    s2_send[...] = acc
    for k in far_z:
        send(s2_send, s2_recv.at[k], "s2", (k,), at(x, (z + k) % nz, c))
    for k in near_z:
        arrived(s2_recv.at[k], "s2", (k,))
        acc = acc + s2_recv[k]
    s3_send[...] = acc

    def score_copy(k):
        return copy_of(s3_send, s3_recv.at[k], "s3", (k,), ((sec + k) % n_sections, dp))


    @pl.when(sec < n_sections - 1)
    def _():
        pl.semaphore_wait(ready, n_sections - 1 - sec)

    for k in far_s:

        @pl.when(sec + k < n_sections)
        def _(k=k):
            score_copy(k).start()

    for k in reversed(far_s):

        @pl.when(sec >= k)
        def _(k=k):
            score_copy(k).wait_recv()

        acc = acc + jnp.where(sec >= k, s3_recv[k], 0.0)

    lane = lax.broadcasted_iota(jnp.int32, (8, 128), 1)
    row = lax.broadcasted_iota(jnp.int32, (8, 128), 0) + dp * 8
    length = jnp.full((8, 128), 1, jnp.int32)
    target = jnp.full((8, 128), -1, jnp.int32)
    for m in range(4):
        inside = lane // 8 == m
        length = jnp.where(inside, len_ref[m], length)
        target = jnp.where(inside, rows_ref[m], target)
    scaled = acc * (1.0 / length.astype(jnp.float32))
    spread = jnp.where(target == row, scaled, 0.0)
    pick = lax.broadcasted_iota(jnp.int32, (128, 128), 0) % 8
    pick = pick == lax.broadcasted_iota(jnp.int32, (128, 128), 1)
    table = jnp.dot(
        spread, pick.astype(jnp.float32), precision=HIGH, preferred_element_type=jnp.float32
    )
    out_ref[...] = prior_ref[...] + table[:, 0:8]
    for copy in pending:
        copy.wait_send()
    for k in far_s:

        @pl.when(sec + k < n_sections)
        def _(k=k):
            score_copy(k).wait_send()


def per_device(n_sections, nz, acts, grads, basis_in, basis_out, eig, query, lengths, rows, prior):
    ff, d = acts.shape[3], grads.shape[3]
    rank = basis_in.shape[2]
    half = rank // 2
    ib = eig.shape[1]
    tokens = 2 * nz * 16
    tz = tokens // nz
    kx, kgx = ff // NX, d // NX
    bf, f32 = jnp.bfloat16, jnp.float32
    dma = pltpu.SemaphoreType.DMA
    vm = pltpu.VMEM
    hbm = pl.BlockSpec(memory_space=pl.ANY)
    vmem = pl.BlockSpec(memory_space=pltpu.VMEM)
    out = pl.pallas_call(
        functools.partial(kernel, n_sections, nz),
        out_shape=jax.ShapeDtypeStruct(prior.shape, f32),
        in_specs=[hbm] * 9,
        out_specs=vmem,
        scratch_shapes=[
            pltpu.SMEM((4,), jnp.int32),
            pltpu.SMEM((4,), jnp.int32),
            vm(prior.shape, f32),
            vm((4, ff), bf),
            vm((4, d), bf),
            vm((ib, rank), f32),
            vm((8, ib, rank), bf),
            vm((WIN, half), bf),
            vm((2 * KG, half), bf),
            vm((half, 2 * KG), bf),
            vm((2 * NX, 8, ib, 128), bf),
            vm((2 * NX, 8, ib, 128), bf),
            vm((NX, 4, kx + kgx), bf),
            vm((nz, 16, WIN), bf),
            vm((nz, 16, 2 * KG), bf),
            vm((nz, 2, 16, WIN), bf),
            vm((nz, 2, 16, 2 * KG), bf),
            vm((nz, NX, tz, 128), bf),
            vm((NX, nz, ib, tokens), bf),
            vm((nz, 2, tz // 2, 128), bf),
            vm((2, nz // 2, ib, tokens), bf),
            vm((nz, 2, tz, 128), bf),
            vm((2, nz, ib, tokens), bf),
            vm((nz, tz, 128), bf),
            vm((nz, ib, tokens), bf),
            vm((nz, tz, 128), bf),
            vm((nz, ib, tokens), bf),
            vm((tz, 128), bf),
            vm((ib, tokens), bf),
            vm((nz, tz, 128), bf),
            vm((2 * NX, ib, tokens), bf),
            vm((128, 128), f32),
            vm((1, 128), f32),
            vm((2 * NX, 1, 128), f32),
            vm((1, 128), f32),
            vm((nz, 1, 128), f32),
            vm((1, 128), f32),
            vm((n_sections, 1, 128), f32),
            dma((11,)),
            pltpu.SemaphoreType.REGULAR,
            dma((2, 2, NX)),
            dma((2, 2, nz)),
            dma((2, 2, nz)),
            dma((2, 2)),
            dma((2, 7)),
            dma((2, 2, nz, 2)),
            dma((2, 2, nz, 2)),
            dma((2, 2, nz)),
            dma((2, nz)),
            dma((2, 7)),
            dma((2, 7)),
            dma((2, nz)),
            dma((2, n_sections)),
        ],
        compiler_params=pltpu.CompilerParams(collective_id=0, has_side_effects=True),
    )(
        acts.reshape(4, ff),
        grads.reshape(4, d),
        basis_in[0],
        basis_out[0],
        eig[0],
        query[0],
        lengths,
        rows,
        prior,
    )
    return out[None]


def solution(mesh):
    n_sections, n_dp = mesh.shape["section"], mesh.shape["dp"]
    return jax.shard_map(
        functools.partial(per_device, n_sections, n_dp // (NX * NC)),
        mesh=mesh,
        in_specs=(
            P("section", None, "dp", None),
            P("section", None, "dp", None),
            P("section", "dp", None),
            P("section", "dp", None),
            P("section", "dp", None),
            P("section", None, "dp", None),
            P(),
            P(),
            P("dp", None),
        ),
        out_specs=P("section", "dp", None),
        check_vma=False,
    )
```

```python
import functools

import jax
import jax.numpy as jnp
from jax import lax
from jax.experimental import pallas as pl
from jax.experimental.pallas import tpu as pltpu
from jax.sharding import PartitionSpec as P

DAMPING = 0.01
MESH = pl.DeviceIdType.MESH
NX = 4
NC = 2
KA = 224
KG = 64
WIN = 512
SEMS = ("x", "z", "c", "bw", "p", "rx", "rz", "az", "gx", "s1", "s2", "s3")
HIGH = lax.Precision.HIGHEST


def far_first(n):
    return sorted(range(1, n), key=lambda k: -min(k, n - k))


def kernel(
    n_sections,
    nz,
    a_hbm,
    g_hbm,
    b_hbm,
    w_hbm,
    e_hbm,
    q_hbm,
    len_hbm,
    rows_hbm,
    prior_hbm,
    out_ref,
    len_ref,
    rows_ref,
    prior_ref,
    a_v,
    g_v,
    e_v,
    q_v,
    b_full,
    w_full,
    w_t,
    p_send,
    p_full,
    x_recv,
    z_send_a,
    z_send_g,
    tok_a,
    tok_g,
    xs_a,
    xs_g,
    xr_a,
    xr_g,
    zs_a,
    zs_g,
    zr_a,
    zr_g,
    ap_own,
    gp_own,
    ap_full,
    gp_full,
    rows_x,
    s1_send,
    s1_recv,
    s2_send,
    s2_recv,
    s3_send,
    s3_recv,
    load_sem,
    ready,
    *sem_refs,
):
    sec = lax.axis_index("section")
    dp = lax.axis_index("dp")
    x = dp // (2 * nz)
    z = (dp % (2 * nz)) // 2
    c = dp % 2
    ib = gp_own.shape[0]
    tz = ap_own.shape[0]
    half = w_full.shape[1]
    kgx = nz * 2 * KG
    kx = x_recv.shape[2] - kgx
    sems = dict(zip(SEMS, sem_refs, strict=True))

    def at(xx, zz, cc):
        return (sec, (xx * nz + zz) * 2 + cc)

    def copy_of(src, dst, name, i, dev):
        return pltpu.make_async_remote_copy(
            src_ref=src,
            dst_ref=dst,
            send_sem=sems[name].at[(0, *i)],
            recv_sem=sems[name].at[(1, *i)],
            device_id=dev,
            device_id_type=MESH,
        )

    def send(src, dst, name, i, dev):
        copy = copy_of(src, dst, name, i, dev)
        copy.start()
        pending.append(copy)

    def arrived(dst, name, i):
        copy_of(dst, dst, name, i, (sec, dp)).wait_recv()

    pending = []
    far_x = far_first(NX)
    far_z = far_first(nz)
    near_z = far_z[::-1]
    far_s = far_first(n_sections)
    group = [(dx, dc) for dx in (2, 1, 3, 0) for dc in (0, 1) if dx or dc]

    barrier = pltpu.get_barrier_semaphore()
    partners = [at((x + dx) % NX, z, (c + dc) % 2) for dx, dc in group]
    partners += [at(x, (z + k) % nz, c) for k in far_z]
    for dev in partners:
        pl.semaphore_signal(barrier, inc=1, device_id=dev, device_id_type=MESH)
    for k in far_s:

        @pl.when(sec + k < n_sections)
        def _(k=k):
            pl.semaphore_signal(barrier, inc=1, device_id=(sec + k, dp), device_id_type=MESH)

    off = pl.multiple_of(64 * (z % 2) + KA * c, 32)
    off_twin = pl.multiple_of(64 * (z % 2) + KA * (1 - c), 32)
    goff = pl.multiple_of(KG * c, 64)
    goff_twin = pl.multiple_of(KG * (1 - c), 64)
    mine = pl.ds(pl.multiple_of(half * c, 128), half)
    other = pl.ds(pl.multiple_of(half * (1 - c), 128), half)
    a_own = a_hbm.at[:, pl.ds(pl.multiple_of(kx * x, 128), kx)]
    g_own = g_hbm.at[:, pl.ds(pl.multiple_of(kgx * x, 128), kgx)]
    loads = [
        pltpu.make_async_copy(s, d, load_sem.at[i])
        for i, (s, d) in enumerate(
            (
                (g_hbm, g_v),
                (a_hbm, a_v),
                (g_own, x_recv.at[x, :, pl.ds(kx, kgx)]),
                (a_own, x_recv.at[x, :, pl.ds(0, kx)]),
                (e_hbm, e_v),
                (q_hbm, q_v),
                (b_hbm.at[:, mine], b_full.at[pl.ds(off, KA), :]),
                (w_hbm.at[:, mine], w_full.at[pl.ds(goff, KG), :]),
                (len_hbm, len_ref),
                (rows_hbm, rows_ref),
                (prior_hbm, prior_ref),
            )
        )
    ]
    for load in loads:
        load.start()

    pl.semaphore_wait(barrier, len(partners) + sec)

    loads[0].wait()
    for k in far_x:
        xx = (x + k) % NX
        send(
            g_v.at[:, pl.ds(pl.multiple_of(kgx * xx, 128), kgx)],
            x_recv.at[x, :, pl.ds(kx, kgx)],
            "x",
            (1, k),
            at(xx, z, c),
        )
    loads[1].wait()
    for k in far_x:
        xx = (x + k) % NX
        send(
            a_v.at[:, pl.ds(pl.multiple_of(kx * xx, 128), kx)],
            x_recv.at[x, :, pl.ds(0, kx)],
            "x",
            (0, k),
            at(xx, z, c),
        )
    twin = at(x, z, 1 - c)
    send(b_hbm.at[:, other], b_full.at[pl.ds(off, KA), :], "bw", (0,), twin)
    send(w_hbm.at[:, other], w_full.at[pl.ds(goff, KG), :], "bw", (1,), twin)

    zero_at = pl.multiple_of((1 - z % 2) * 2 * KA, 64)
    b_full[pl.ds(zero_at, 64), :] = jnp.zeros((64, half), jnp.bfloat16)
    rows_x[...] = jnp.zeros_like(rows_x)
    loads[4].wait()
    loads[5].wait()
    for b in range(2 * NX):
        cols = slice(128 * b, 128 * b + 128)
        den = e_v[:, cols] + DAMPING
        num = q_v[:, :, cols].astype(jnp.float32)
        p_send[b] = (num / den[None]).astype(jnp.bfloat16)
    p_full[2 * x + c] = p_send[4 * c + x]

    loads[2].wait()
    for k in far_x:
        arrived(x_recv.at[(x + NX - k) % NX, :, pl.ds(kx, kgx)], "x", (1, k))
    for zz in range(nz):
        gs = kx + 2 * KG * zz
        z_send_g[zz] = jnp.concatenate(
            [x_recv[i, :, gs : gs + 2 * KG] for i in range(NX)], axis=0
        )
    for k in far_z:
        zz = (z + k) % nz
        send(z_send_g.at[zz], tok_g.at[z, c], "z", (1, k), at(x, zz, c))
    send(z_send_g.at[z], tok_g.at[z, c], "c", (1, 0), twin)
    tok_g[z, c] = z_send_g[z]
    loads[3].wait()
    for k in far_x:
        arrived(x_recv.at[(x + NX - k) % NX, :, pl.ds(0, kx)], "x", (0, k))
    for zz in range(nz):
        start = 896 * (zz // 2) + 384 * (zz % 2)
        z_send_a[zz] = jnp.concatenate(
            [x_recv[i, :, start : start + WIN] for i in range(NX)], axis=0
        )
    for k in far_z:
        zz = (z + k) % nz
        send(z_send_a.at[zz], tok_a.at[z, c], "z", (0, k), at(x, zz, c))
    send(z_send_a.at[z], tok_a.at[z, c], "c", (0, 0), twin)
    tok_a[z, c] = z_send_a[z]
    for i, (dx, dc) in enumerate(group):
        xx, cc = (x + dx) % NX, (c + dc) % 2
        send(p_send.at[4 * cc + xx], p_full.at[2 * x + c], "p", (i,), at(xx, z, cc))

    for k in far_s:

        @pl.when(sec >= k)
        def _(k=k):
            pl.semaphore_signal(ready, inc=1, device_id=(sec - k, dp), device_id_type=MESH)

    loads[6].wait()
    loads[7].wait()
    arrived(w_full.at[pl.ds(goff_twin, KG), :], "bw", (1,))
    w_t[...] = w_full[...].astype(jnp.float32).T.astype(jnp.bfloat16)
    arrived(b_full.at[pl.ds(off_twin, KA), :], "bw", (0,))

    tokens = nz * tz

    def forward(tok, kind, k):
        zz = (z + nz - k) % nz
        arrived(tok.at[zz, c], "z", (kind, k))
        send(tok.at[zz, c], tok.at[zz, c], "c", (kind, k), twin)

    def project_acts(k):
        zz = (z + nz - k) % nz
        arrived(tok_a.at[zz, 1 - c], "c", (0, k))
        part = jnp.dot(
            tok_a[zz].reshape(tz, WIN), b_full[...], preferred_element_type=jnp.float32
        ).astype(jnp.bfloat16)
        for i in range(NX):
            xs_a[zz, i] = part[:, 128 * i : 128 * i + 128]
        for kx_ in far_x:
            xx = (x + kx_) % NX
            send(xs_a.at[zz, xx], xr_a.at[zz, x], "rx", (0, k, kx_), at(xx, z, c))

    def project_grads():
        for k in [0] + near_z:
            arrived(tok_g.at[(z + nz - k) % nz, 1 - c], "c", (1, k))
        part = lax.dot_general(
            w_t[...],
            tok_g[...].reshape(tokens, 2 * KG),
            (((1,), (1,)), ((), ())),
            preferred_element_type=jnp.float32,
        ).astype(jnp.bfloat16)
        for i in range(NX):
            for zz in range(nz):
                r = (i // 2) * 2 * nz * ib + zz * 2 * ib + (i % 2) * ib
                xs_g[zz, i] = part[r : r + ib, :]
        for k in far_z + [0]:
            zz = (z + k) % nz
            for kx_ in far_x:
                xx = (x + kx_) % NX
                send(xs_g.at[zz, xx], xr_g.at[zz, x], "rx", (1, k, kx_), at(xx, z, c))

    def sum_over_x(sent, recv, out, kind, k, zz):
        total = sent[zz, x].astype(jnp.float32)
        for kx_ in far_x:
            xx = (x + NX - kx_) % NX
            arrived(recv.at[zz, xx], "rx", (kind, k, kx_))
            total = total + recv[zz, xx].astype(jnp.float32)
        out[zz] = total.astype(jnp.bfloat16)

    def sum_over_z(sums, recv, kind):
        total = sums[z].astype(jnp.float32)
        for k in near_z:
            zz = (z + nz - k) % nz
            arrived(recv.at[zz], "rz", (kind, k))
            total = total + recv[zz].astype(jnp.float32)
        return total.astype(jnp.bfloat16)

    order = [0] + near_z
    for k in near_z:
        forward(tok_g, 1, k)
    for k in near_z:
        forward(tok_a, 0, k)
    project_grads()
    for k in order:
        project_acts(k)

    for k in far_z + [0]:
        zz = (z + k) % nz
        sum_over_x(xs_g, xr_g, zs_g, 1, k, zz)
        if k:
            send(zs_g.at[zz], zr_g.at[z], "rz", (1, k), at(x, zz, c))
    for k in order:
        zz = (z + nz - k) % nz
        sum_over_x(xs_a, xr_a, zs_a, 0, k, zz)
        if k:
            send(zs_a.at[zz], zr_a.at[z], "rz", (0, nz - k), at(x, zz, c))
    own = sum_over_z(zs_g, zr_g, 1)
    gp_own[...] = own
    for i, (dx, dc) in enumerate(group):
        xx, cc = (x + dx) % NX, (c + dc) % 2
        send(gp_own, gp_full.at[4 * c + x], "gx", (i,), at(xx, z, cc))
    gp_full[4 * c + x] = own
    own = sum_over_z(zs_a, zr_a, 0)
    ap_own[...] = own
    for k in far_z:
        send(ap_own, ap_full.at[z], "az", (k,), at(x, (z + k) % nz, c))
    ap_full[z] = own

    for i, (dx, dc) in enumerate(group):
        xx, cc = (x + NX - dx) % NX, (c + 2 - dc) % 2
        arrived(p_full.at[2 * xx + cc], "p", (i,))
        arrived(gp_full.at[4 * cc + xx], "gx", (i,))
    for k in near_z:
        arrived(ap_full.at[(z + nz - k) % nz], "az", (k,))
    for load in loads[8:]:
        load.wait()
    lane = lax.broadcasted_iota(jnp.int32, (8 * ib, tokens), 1)
    micro = lane % 4
    slot = ((lane // 4) % 4) * 2 * nz + (lane // tz) * 2 + (lane // 16) % 2
    gp = gp_full[...].reshape(8 * ib, tokens).astype(jnp.float32)
    ap = ap_full[...].reshape(tokens, 128)
    for m in range(4):
        live = jnp.where(micro == m, slot, 2**20) < len_ref[m]
        seq = jnp.dot(
            jnp.where(live, gp, 0.0).astype(jnp.bfloat16), ap, preferred_element_type=jnp.float32
        )
        for q in range(8):
            row = seq * p_full[:, q].reshape(8 * ib, 128).astype(jnp.float32)
            rows_x[m * 8 + q : m * 8 + q + 1, :] = jnp.sum(row, axis=0, keepdims=True)
    score = lax.dot_general(
        jnp.ones((8, 128), jnp.float32),
        rows_x[...],
        (((1,), (1,)), ((), ())),
        precision=HIGH,
        preferred_element_type=jnp.float32,
    )
    s1_send[...] = score[0:1, :]
    for i, (dx, dc) in enumerate(group):
        xx, cc = (x + dx) % NX, (c + dc) % 2
        send(s1_send, s1_recv.at[i], "s1", (i,), at(xx, z, cc))
    acc = score[0:1, :]
    for i in range(len(group)):
        arrived(s1_recv.at[i], "s1", (i,))
        acc = acc + s1_recv[i]
    s2_send[...] = acc
    for k in far_z:
        send(s2_send, s2_recv.at[k], "s2", (k,), at(x, (z + k) % nz, c))
    for k in near_z:
        arrived(s2_recv.at[k], "s2", (k,))
        acc = acc + s2_recv[k]
    s3_send[...] = acc

    def score_copy(k):
        return copy_of(s3_send, s3_recv.at[k], "s3", (k,), ((sec + k) % n_sections, dp))


    @pl.when(sec < n_sections - 1)
    def _():
        pl.semaphore_wait(ready, n_sections - 1 - sec)

    for k in far_s:

        @pl.when(sec + k < n_sections)
        def _(k=k):
            score_copy(k).start()

    for k in reversed(far_s):

        @pl.when(sec >= k)
        def _(k=k):
            score_copy(k).wait_recv()

        acc = acc + jnp.where(sec >= k, s3_recv[k], 0.0)

    lane = lax.broadcasted_iota(jnp.int32, (8, 128), 1)
    row = lax.broadcasted_iota(jnp.int32, (8, 128), 0) + dp * 8
    length = jnp.full((8, 128), 1, jnp.int32)
    target = jnp.full((8, 128), -1, jnp.int32)
    for m in range(4):
        inside = lane // 8 == m
        length = jnp.where(inside, len_ref[m], length)
        target = jnp.where(inside, rows_ref[m], target)
    scaled = acc * (1.0 / length.astype(jnp.float32))
    spread = jnp.where(target == row, scaled, 0.0)
    pick = lax.broadcasted_iota(jnp.int32, (128, 128), 0) % 8
    pick = pick == lax.broadcasted_iota(jnp.int32, (128, 128), 1)
    table = jnp.dot(
        spread, pick.astype(jnp.float32), precision=HIGH, preferred_element_type=jnp.float32
    )
    out_ref[...] = prior_ref[...] + table[:, 0:8]
    for copy in pending:
        copy.wait_send()
    for k in far_s:

        @pl.when(sec + k < n_sections)
        def _(k=k):
            score_copy(k).wait_send()


def per_device(n_sections, nz, acts, grads, basis_in, basis_out, eig, query, lengths, rows, prior):
    ff, d = acts.shape[3], grads.shape[3]
    rank = basis_in.shape[2]
    half = rank // 2
    ib = eig.shape[1]
    tokens = 2 * nz * 16
    tz = tokens // nz
    kx, kgx = ff // NX, d // NX
    bf, f32 = jnp.bfloat16, jnp.float32
    dma = pltpu.SemaphoreType.DMA
    vm = pltpu.VMEM
    hbm = pl.BlockSpec(memory_space=pl.ANY)
    vmem = pl.BlockSpec(memory_space=pltpu.VMEM)
    out = pl.pallas_call(
        functools.partial(kernel, n_sections, nz),
        out_shape=jax.ShapeDtypeStruct(prior.shape, f32),
        in_specs=[hbm] * 9,
        out_specs=vmem,
        scratch_shapes=[
            pltpu.SMEM((4,), jnp.int32),
            pltpu.SMEM((4,), jnp.int32),
            vm(prior.shape, f32),
            vm((4, ff), bf),
            vm((4, d), bf),
            vm((ib, rank), f32),
            vm((8, ib, rank), bf),
            vm((WIN, half), bf),
            vm((2 * KG, half), bf),
            vm((half, 2 * KG), bf),
            vm((2 * NX, 8, ib, 128), bf),
            vm((2 * NX, 8, ib, 128), bf),
            vm((NX, 4, kx + kgx), bf),
            vm((nz, 16, WIN), bf),
            vm((nz, 16, 2 * KG), bf),
            vm((nz, 2, 16, WIN), bf),
            vm((nz, 2, 16, 2 * KG), bf),
            vm((nz, NX, tz, 128), bf),
            vm((nz, NX, ib, tokens), bf),
            vm((nz, NX, tz, 128), bf),
            vm((nz, NX, ib, tokens), bf),
            vm((nz, tz, 128), bf),
            vm((nz, ib, tokens), bf),
            vm((nz, tz, 128), bf),
            vm((nz, ib, tokens), bf),
            vm((tz, 128), bf),
            vm((ib, tokens), bf),
            vm((nz, tz, 128), bf),
            vm((2 * NX, ib, tokens), bf),
            vm((128, 128), f32),
            vm((1, 128), f32),
            vm((2 * NX, 1, 128), f32),
            vm((1, 128), f32),
            vm((nz, 1, 128), f32),
            vm((1, 128), f32),
            vm((n_sections, 1, 128), f32),
            dma((11,)),
            pltpu.SemaphoreType.REGULAR,
            dma((2, 2, NX)),
            dma((2, 2, nz)),
            dma((2, 2, nz)),
            dma((2, 2)),
            dma((2, 7)),
            dma((2, 2, nz, NX)),
            dma((2, 2, nz)),
            dma((2, nz)),
            dma((2, 7)),
            dma((2, 7)),
            dma((2, nz)),
            dma((2, n_sections)),
        ],
        compiler_params=pltpu.CompilerParams(collective_id=0, has_side_effects=True),
    )(
        acts.reshape(4, ff),
        grads.reshape(4, d),
        basis_in[0],
        basis_out[0],
        eig[0],
        query[0],
        lengths,
        rows,
        prior,
    )
    return out[None]


def solution(mesh):
    n_sections, n_dp = mesh.shape["section"], mesh.shape["dp"]
    return jax.shard_map(
        functools.partial(per_device, n_sections, n_dp // (NX * NC)),
        mesh=mesh,
        in_specs=(
            P("section", None, "dp", None),
            P("section", None, "dp", None),
            P("section", "dp", None),
            P("section", "dp", None),
            P("section", "dp", None),
            P("section", None, "dp", None),
            P(),
            P(),
            P("dp", None),
        ),
        out_specs=P("section", "dp", None),
        check_vma=False,
    )
```

```python
import functools

import jax
import jax.numpy as jnp
from jax import lax
from jax.experimental import pallas as pl
from jax.experimental.pallas import tpu as pltpu
from jax.sharding import PartitionSpec as P

DAMPING = 0.01
MESH = pl.DeviceIdType.MESH
NX = 4
NC = 2
KA = 224
KG = 64
WIN = 512
SEMS = ("x", "z", "c", "bw", "p", "rx", "rz", "az", "gx", "s1", "s2", "s3")
HIGH = lax.Precision.HIGHEST


def far_first(n):
    return sorted(range(1, n), key=lambda k: -min(k, n - k))


def kernel(
    n_sections,
    nz,
    a_hbm,
    g_hbm,
    b_hbm,
    w_hbm,
    e_hbm,
    q_hbm,
    len_hbm,
    rows_hbm,
    prior_hbm,
    out_ref,
    len_ref,
    rows_ref,
    prior_ref,
    a_v,
    g_v,
    e_v,
    q_v,
    b_full,
    w_full,
    w_t,
    p_send,
    p_full,
    x_recv,
    z_send_a,
    z_send_g,
    tok_a,
    tok_g,
    xs_a,
    xs_g,
    xr_a,
    xr_g,
    zs_a,
    zs_g,
    zr_a,
    zr_g,
    ap_own,
    gp_own,
    ap_full,
    gp_full,
    rows_x,
    s1_send,
    s1_recv,
    s2_send,
    s2_recv,
    s3_send,
    s3_recv,
    load_sem,
    ready,
    *sem_refs,
):
    sec = lax.axis_index("section")
    dp = lax.axis_index("dp")
    x = dp // (2 * nz)
    z = (dp % (2 * nz)) // 2
    c = dp % 2
    ib = gp_own.shape[0]
    tz = ap_own.shape[0]
    half = w_full.shape[1]
    kgx = nz * 2 * KG
    kx = x_recv.shape[2] - kgx
    sems = dict(zip(SEMS, sem_refs, strict=True))

    def at(xx, zz, cc):
        return (sec, (xx * nz + zz) * 2 + cc)

    def copy_of(src, dst, name, i, dev):
        return pltpu.make_async_remote_copy(
            src_ref=src,
            dst_ref=dst,
            send_sem=sems[name].at[(0, *i)],
            recv_sem=sems[name].at[(1, *i)],
            device_id=dev,
            device_id_type=MESH,
        )

    def send(src, dst, name, i, dev):
        copy = copy_of(src, dst, name, i, dev)
        copy.start()
        pending.append(copy)

    def arrived(dst, name, i):
        copy_of(dst, dst, name, i, (sec, dp)).wait_recv()

    pending = []
    far_x = far_first(NX)
    far_z = far_first(nz)
    near_z = far_z[::-1]
    far_s = far_first(n_sections)
    group = [(dx, dc) for dx in (2, 1, 3, 0) for dc in (0, 1) if dx or dc]

    barrier = pltpu.get_barrier_semaphore()
    partners = [at((x + dx) % NX, z, (c + dc) % 2) for dx, dc in group]
    partners += [at(x, (z + k) % nz, c) for k in far_z]
    for dev in partners:
        pl.semaphore_signal(barrier, inc=1, device_id=dev, device_id_type=MESH)
    for k in far_s:

        @pl.when(sec + k < n_sections)
        def _(k=k):
            pl.semaphore_signal(barrier, inc=1, device_id=(sec + k, dp), device_id_type=MESH)

    off = pl.multiple_of(64 * (z % 2) + KA * c, 32)
    off_twin = pl.multiple_of(64 * (z % 2) + KA * (1 - c), 32)
    goff = pl.multiple_of(KG * c, 64)
    goff_twin = pl.multiple_of(KG * (1 - c), 64)
    mine = pl.ds(pl.multiple_of(half * c, 128), half)
    other = pl.ds(pl.multiple_of(half * (1 - c), 128), half)
    a_own = a_hbm.at[:, pl.ds(pl.multiple_of(kx * x, 128), kx)]
    g_own = g_hbm.at[:, pl.ds(pl.multiple_of(kgx * x, 128), kgx)]
    loads = [
        pltpu.make_async_copy(s, d, load_sem.at[i])
        for i, (s, d) in enumerate(
            (
                (g_hbm, g_v),
                (a_hbm, a_v),
                (g_own, x_recv.at[x, :, pl.ds(kx, kgx)]),
                (a_own, x_recv.at[x, :, pl.ds(0, kx)]),
                (e_hbm, e_v),
                (q_hbm, q_v),
                (b_hbm.at[:, mine], b_full.at[pl.ds(off, KA), :]),
                (w_hbm.at[:, mine], w_full.at[pl.ds(goff, KG), :]),
                (len_hbm, len_ref),
                (rows_hbm, rows_ref),
                (prior_hbm, prior_ref),
            )
        )
    ]
    for load in loads:
        load.start()

    pl.semaphore_wait(barrier, len(partners) + sec)

    loads[0].wait()
    for k in far_x:
        xx = (x + k) % NX
        send(
            g_v.at[:, pl.ds(pl.multiple_of(kgx * xx, 128), kgx)],
            x_recv.at[x, :, pl.ds(kx, kgx)],
            "x",
            (1, k),
            at(xx, z, c),
        )
    loads[1].wait()
    for k in far_x:
        xx = (x + k) % NX
        send(
            a_v.at[:, pl.ds(pl.multiple_of(kx * xx, 128), kx)],
            x_recv.at[x, :, pl.ds(0, kx)],
            "x",
            (0, k),
            at(xx, z, c),
        )
    twin = at(x, z, 1 - c)
    send(b_hbm.at[:, other], b_full.at[pl.ds(off, KA), :], "bw", (0,), twin)
    send(w_hbm.at[:, other], w_full.at[pl.ds(goff, KG), :], "bw", (1,), twin)

    zero_at = pl.multiple_of((1 - z % 2) * 2 * KA, 64)
    b_full[pl.ds(zero_at, 64), :] = jnp.zeros((64, half), jnp.bfloat16)
    rows_x[...] = jnp.zeros_like(rows_x)
    loads[4].wait()
    loads[5].wait()
    for b in range(2 * NX):
        cols = slice(128 * b, 128 * b + 128)
        den = e_v[:, cols] + DAMPING
        num = q_v[:, :, cols].astype(jnp.float32)
        p_send[b] = (num / den[None]).astype(jnp.bfloat16)
    p_full[2 * x + c] = p_send[4 * c + x]

    loads[2].wait()
    for k in far_x:
        arrived(x_recv.at[(x + NX - k) % NX, :, pl.ds(kx, kgx)], "x", (1, k))
    for zz in range(nz):
        gs = kx + 2 * KG * zz
        z_send_g[zz] = jnp.concatenate(
            [x_recv[i, :, gs : gs + 2 * KG] for i in range(NX)], axis=0
        )
    for k in far_z:
        zz = (z + k) % nz
        send(z_send_g.at[zz], tok_g.at[z, c], "z", (1, k), at(x, zz, c))
    send(z_send_g.at[z], tok_g.at[z, c], "c", (1, 0), twin)
    tok_g[z, c] = z_send_g[z]
    loads[3].wait()
    for k in far_x:
        arrived(x_recv.at[(x + NX - k) % NX, :, pl.ds(0, kx)], "x", (0, k))
    for zz in range(nz):
        start = 896 * (zz // 2) + 384 * (zz % 2)
        z_send_a[zz] = jnp.concatenate(
            [x_recv[i, :, start : start + WIN] for i in range(NX)], axis=0
        )
    for k in far_z:
        zz = (z + k) % nz
        send(z_send_a.at[zz], tok_a.at[z, c], "z", (0, k), at(x, zz, c))
    send(z_send_a.at[z], tok_a.at[z, c], "c", (0, 0), twin)
    tok_a[z, c] = z_send_a[z]
    for i, (dx, dc) in enumerate(group):
        xx, cc = (x + dx) % NX, (c + dc) % 2
        send(p_send.at[4 * cc + xx], p_full.at[2 * x + c], "p", (i,), at(xx, z, cc))

    for k in far_s:

        @pl.when(sec >= k)
        def _(k=k):
            pl.semaphore_signal(ready, inc=1, device_id=(sec - k, dp), device_id_type=MESH)

    loads[6].wait()
    loads[7].wait()
    arrived(w_full.at[pl.ds(goff_twin, KG), :], "bw", (1,))
    w_t[...] = w_full[...].astype(jnp.float32).T.astype(jnp.bfloat16)
    arrived(b_full.at[pl.ds(off_twin, KA), :], "bw", (0,))

    tokens = nz * tz

    def forward(tok, kind, k):
        zz = (z + nz - k) % nz
        arrived(tok.at[zz, c], "z", (kind, k))
        send(tok.at[zz, c], tok.at[zz, c], "c", (kind, k), twin)

    def project_acts(k):
        zz = (z + nz - k) % nz
        arrived(tok_a.at[zz, 1 - c], "c", (0, k))
        part = jnp.dot(
            tok_a[zz].reshape(tz, WIN), b_full[...], preferred_element_type=jnp.float32
        ).astype(jnp.bfloat16)
        for i in range(NX):
            xs_a[zz, i] = part[:, 128 * i : 128 * i + 128]
        for kx_ in far_x:
            xx = (x + kx_) % NX
            send(xs_a.at[zz, xx], xr_a.at[zz, x], "rx", (0, k, kx_), at(xx, z, c))

    def project_grads():
        for k in [0] + near_z:
            arrived(tok_g.at[(z + nz - k) % nz, 1 - c], "c", (1, k))
        part = lax.dot_general(
            w_t[...],
            tok_g[...].reshape(tokens, 2 * KG),
            (((1,), (1,)), ((), ())),
            preferred_element_type=jnp.float32,
        ).astype(jnp.bfloat16)
        for i in range(NX):
            for zz in range(nz):
                r = (i // 2) * 2 * nz * ib + zz * 2 * ib + (i % 2) * ib
                xs_g[zz, i] = part[r : r + ib, :]
        for k in far_z:
            zz = (z + k) % nz
            send(xs_g.at[zz], zr_g.at[z], "rz", (1, k), at(x, zz, c))

    def sum_over_x(own, recv, kind, k):
        total = own.astype(jnp.float32)
        for kx_ in far_x:
            xx = (x + NX - kx_) % NX
            arrived(recv.at[xx], "rx", (kind, k, kx_))
            total = total + recv[xx].astype(jnp.float32)
        return total.astype(jnp.bfloat16)

    def sum_over_z(sums, recv, kind):
        total = sums[z].astype(jnp.float32)
        for k in near_z:
            zz = (z + nz - k) % nz
            arrived(recv.at[zz], "rz", (kind, k))
            total = total + recv[zz].astype(jnp.float32)
        return total.astype(jnp.bfloat16)

    order = [0] + near_z
    for k in near_z:
        forward(tok_g, 1, k)
    for k in near_z:
        forward(tok_a, 0, k)
    project_grads()
    for k in order:
        project_acts(k)

    for k in order:
        zz = (z + nz - k) % nz
        zs_a[zz] = sum_over_x(xs_a[zz, x], xr_a.at[zz], 0, k)
        if k:
            send(zs_a.at[zz], zr_a.at[z], "rz", (0, nz - k), at(x, zz, c))
    zs_g[...] = sum_over_z(xs_g, zr_g, 1)
    for kx_ in far_x:
        xx = (x + kx_) % NX
        send(zs_g.at[xx], xr_g.at[x], "rx", (1, 0, kx_), at(xx, z, c))
    own = sum_over_z(zs_a, zr_a, 0)
    ap_own[...] = own
    for k in far_z:
        send(ap_own, ap_full.at[z], "az", (k,), at(x, (z + k) % nz, c))
    ap_full[z] = own
    own = sum_over_x(zs_g[x], xr_g, 1, 0)
    gp_own[...] = own
    for i, (dx, dc) in enumerate(group):
        xx, cc = (x + dx) % NX, (c + dc) % 2
        send(gp_own, gp_full.at[4 * c + x], "gx", (i,), at(xx, z, cc))
    gp_full[4 * c + x] = own

    for i, (dx, dc) in enumerate(group):
        xx, cc = (x + NX - dx) % NX, (c + 2 - dc) % 2
        arrived(p_full.at[2 * xx + cc], "p", (i,))
        arrived(gp_full.at[4 * cc + xx], "gx", (i,))
    for k in near_z:
        arrived(ap_full.at[(z + nz - k) % nz], "az", (k,))
    for load in loads[8:]:
        load.wait()
    lane = lax.broadcasted_iota(jnp.int32, (8 * ib, tokens), 1)
    micro = lane % 4
    slot = ((lane // 4) % 4) * 2 * nz + (lane // tz) * 2 + (lane // 16) % 2
    gp = gp_full[...].reshape(8 * ib, tokens).astype(jnp.float32)
    ap = ap_full[...].reshape(tokens, 128)
    for m in range(4):
        live = jnp.where(micro == m, slot, 2**20) < len_ref[m]
        seq = jnp.dot(
            jnp.where(live, gp, 0.0).astype(jnp.bfloat16), ap, preferred_element_type=jnp.float32
        )
        for q in range(8):
            row = seq * p_full[:, q].reshape(8 * ib, 128).astype(jnp.float32)
            rows_x[m * 8 + q : m * 8 + q + 1, :] = jnp.sum(row, axis=0, keepdims=True)
    score = lax.dot_general(
        jnp.ones((8, 128), jnp.float32),
        rows_x[...],
        (((1,), (1,)), ((), ())),
        precision=HIGH,
        preferred_element_type=jnp.float32,
    )
    s1_send[...] = score[0:1, :]
    for i, (dx, dc) in enumerate(group):
        xx, cc = (x + dx) % NX, (c + dc) % 2
        send(s1_send, s1_recv.at[i], "s1", (i,), at(xx, z, cc))
    acc = score[0:1, :]
    for i in range(len(group)):
        arrived(s1_recv.at[i], "s1", (i,))
        acc = acc + s1_recv[i]
    s2_send[...] = acc
    for k in far_z:
        send(s2_send, s2_recv.at[k], "s2", (k,), at(x, (z + k) % nz, c))
    for k in near_z:
        arrived(s2_recv.at[k], "s2", (k,))
        acc = acc + s2_recv[k]
    s3_send[...] = acc

    def score_copy(k):
        return copy_of(s3_send, s3_recv.at[k], "s3", (k,), ((sec + k) % n_sections, dp))


    @pl.when(sec < n_sections - 1)
    def _():
        pl.semaphore_wait(ready, n_sections - 1 - sec)

    for k in far_s:

        @pl.when(sec + k < n_sections)
        def _(k=k):
            score_copy(k).start()

    for k in reversed(far_s):

        @pl.when(sec >= k)
        def _(k=k):
            score_copy(k).wait_recv()

        acc = acc + jnp.where(sec >= k, s3_recv[k], 0.0)

    lane = lax.broadcasted_iota(jnp.int32, (8, 128), 1)
    row = lax.broadcasted_iota(jnp.int32, (8, 128), 0) + dp * 8
    length = jnp.full((8, 128), 1, jnp.int32)
    target = jnp.full((8, 128), -1, jnp.int32)
    for m in range(4):
        inside = lane // 8 == m
        length = jnp.where(inside, len_ref[m], length)
        target = jnp.where(inside, rows_ref[m], target)
    scaled = acc * (1.0 / length.astype(jnp.float32))
    spread = jnp.where(target == row, scaled, 0.0)
    pick = lax.broadcasted_iota(jnp.int32, (128, 128), 0) % 8
    pick = pick == lax.broadcasted_iota(jnp.int32, (128, 128), 1)
    table = jnp.dot(
        spread, pick.astype(jnp.float32), precision=HIGH, preferred_element_type=jnp.float32
    )
    out_ref[...] = prior_ref[...] + table[:, 0:8]
    for copy in pending:
        copy.wait_send()
    for k in far_s:

        @pl.when(sec + k < n_sections)
        def _(k=k):
            score_copy(k).wait_send()


def per_device(n_sections, nz, acts, grads, basis_in, basis_out, eig, query, lengths, rows, prior):
    ff, d = acts.shape[3], grads.shape[3]
    rank = basis_in.shape[2]
    half = rank // 2
    ib = eig.shape[1]
    tokens = 2 * nz * 16
    tz = tokens // nz
    kx, kgx = ff // NX, d // NX
    bf, f32 = jnp.bfloat16, jnp.float32
    dma = pltpu.SemaphoreType.DMA
    vm = pltpu.VMEM
    hbm = pl.BlockSpec(memory_space=pl.ANY)
    vmem = pl.BlockSpec(memory_space=pltpu.VMEM)
    out = pl.pallas_call(
        functools.partial(kernel, n_sections, nz),
        out_shape=jax.ShapeDtypeStruct(prior.shape, f32),
        in_specs=[hbm] * 9,
        out_specs=vmem,
        scratch_shapes=[
            pltpu.SMEM((4,), jnp.int32),
            pltpu.SMEM((4,), jnp.int32),
            vm(prior.shape, f32),
            vm((4, ff), bf),
            vm((4, d), bf),
            vm((ib, rank), f32),
            vm((8, ib, rank), bf),
            vm((WIN, half), bf),
            vm((2 * KG, half), bf),
            vm((half, 2 * KG), bf),
            vm((2 * NX, 8, ib, 128), bf),
            vm((2 * NX, 8, ib, 128), bf),
            vm((NX, 4, kx + kgx), bf),
            vm((nz, 16, WIN), bf),
            vm((nz, 16, 2 * KG), bf),
            vm((nz, 2, 16, WIN), bf),
            vm((nz, 2, 16, 2 * KG), bf),
            vm((nz, NX, tz, 128), bf),
            vm((nz, NX, ib, tokens), bf),
            vm((nz, NX, tz, 128), bf),
            vm((NX, ib, tokens), bf),
            vm((nz, tz, 128), bf),
            vm((NX, ib, tokens), bf),
            vm((nz, tz, 128), bf),
            vm((nz, NX, ib, tokens), bf),
            vm((tz, 128), bf),
            vm((ib, tokens), bf),
            vm((nz, tz, 128), bf),
            vm((2 * NX, ib, tokens), bf),
            vm((128, 128), f32),
            vm((1, 128), f32),
            vm((2 * NX, 1, 128), f32),
            vm((1, 128), f32),
            vm((nz, 1, 128), f32),
            vm((1, 128), f32),
            vm((n_sections, 1, 128), f32),
            dma((11,)),
            pltpu.SemaphoreType.REGULAR,
            dma((2, 2, NX)),
            dma((2, 2, nz)),
            dma((2, 2, nz)),
            dma((2, 2)),
            dma((2, 7)),
            dma((2, 2, nz, NX)),
            dma((2, 2, nz)),
            dma((2, nz)),
            dma((2, 7)),
            dma((2, 7)),
            dma((2, nz)),
            dma((2, n_sections)),
        ],
        compiler_params=pltpu.CompilerParams(collective_id=0, has_side_effects=True),
    )(
        acts.reshape(4, ff),
        grads.reshape(4, d),
        basis_in[0],
        basis_out[0],
        eig[0],
        query[0],
        lengths,
        rows,
        prior,
    )
    return out[None]


def solution(mesh):
    n_sections, n_dp = mesh.shape["section"], mesh.shape["dp"]
    return jax.shard_map(
        functools.partial(per_device, n_sections, n_dp // (NX * NC)),
        mesh=mesh,
        in_specs=(
            P("section", None, "dp", None),
            P("section", None, "dp", None),
            P("section", "dp", None),
            P("section", "dp", None),
            P("section", "dp", None),
            P("section", None, "dp", None),
            P(),
            P(),
            P("dp", None),
        ),
        out_specs=P("section", "dp", None),
        check_vma=False,
    )
```

```python
import functools

import jax
import jax.numpy as jnp
from jax import lax
from jax.experimental import pallas as pl
from jax.experimental.pallas import tpu as pltpu
from jax.sharding import PartitionSpec as P

DAMPING = 0.01
MESH = pl.DeviceIdType.MESH
NX = 4
NC = 2
KA = 224
KG = 64
WIN = 512
SEMS = ("x", "z", "c", "bw", "p", "rx", "rz", "az", "gx", "s1", "s3", "fin")
HIGH = lax.Precision.HIGHEST


def far_first(n):
    return sorted(range(1, n), key=lambda k: -min(k, n - k))


def kernel(
    n_sections,
    nz,
    a_hbm,
    g_hbm,
    b_hbm,
    w_hbm,
    e_hbm,
    q_hbm,
    len_hbm,
    rows_hbm,
    prior_hbm,
    out_ref,
    len_ref,
    rows_ref,
    prior_ref,
    a_v,
    g_v,
    e_v,
    q_v,
    b_full,
    w_full,
    w_t,
    p_send,
    p_full,
    x_recv,
    z_send_a,
    z_send_g,
    tok_a,
    tok_g,
    xs_a,
    xs_g,
    xr_a,
    xr_g,
    zs_a,
    zs_g,
    zr_a,
    zr_g,
    ap_own,
    gp_own,
    ap_full,
    gp_full,
    rows_x,
    s1_send,
    s1_recv,
    s3_send,
    s3_recv,
    acc_ref,
    load_sem,
    ready,
    *sem_refs,
):
    sec = lax.axis_index("section")
    dp = lax.axis_index("dp")
    x = dp // (2 * nz)
    z = (dp % (2 * nz)) // 2
    c = dp % 2
    ib = gp_own.shape[0]
    tz = ap_own.shape[0]
    half = w_full.shape[1]
    kgx = nz * 2 * KG
    kx = x_recv.shape[2] - kgx
    sems = dict(zip(SEMS, sem_refs, strict=True))

    def at(xx, zz, cc):
        return (sec, (xx * nz + zz) * 2 + cc)

    def copy_of(src, dst, name, i, dev):
        return pltpu.make_async_remote_copy(
            src_ref=src,
            dst_ref=dst,
            send_sem=sems[name].at[(0, *i)],
            recv_sem=sems[name].at[(1, *i)],
            device_id=dev,
            device_id_type=MESH,
        )

    def send(src, dst, name, i, dev):
        copy = copy_of(src, dst, name, i, dev)
        copy.start()
        pending.append(copy)

    def arrived(dst, name, i):
        copy_of(dst, dst, name, i, (sec, dp)).wait_recv()

    pending = []
    far_x = far_first(NX)
    far_z = far_first(nz)
    near_z = far_z[::-1]
    far_s = far_first(n_sections)
    group = [(dx, dc) for dx in (2, 1, 3, 0) for dc in (0, 1) if dx or dc]

    barrier = pltpu.get_barrier_semaphore()
    partners = [at((x + dx) % NX, z, (c + dc) % 2) for dx, dc in group]
    partners += [at(x, (z + k) % nz, c) for k in far_z]
    for dev in partners:
        pl.semaphore_signal(barrier, inc=1, device_id=dev, device_id_type=MESH)
    for k in far_s:

        @pl.when(sec + k < n_sections)
        def _(k=k):
            pl.semaphore_signal(barrier, inc=1, device_id=(sec + k, dp), device_id_type=MESH)

    off = pl.multiple_of(64 * (z % 2) + KA * c, 32)
    off_twin = pl.multiple_of(64 * (z % 2) + KA * (1 - c), 32)
    goff = pl.multiple_of(KG * c, 64)
    goff_twin = pl.multiple_of(KG * (1 - c), 64)
    mine = pl.ds(pl.multiple_of(half * c, 128), half)
    other = pl.ds(pl.multiple_of(half * (1 - c), 128), half)
    a_own = a_hbm.at[:, pl.ds(pl.multiple_of(kx * x, 128), kx)]
    g_own = g_hbm.at[:, pl.ds(pl.multiple_of(kgx * x, 128), kgx)]
    loads = [
        pltpu.make_async_copy(s, d, load_sem.at[i])
        for i, (s, d) in enumerate(
            (
                (g_hbm, g_v),
                (a_hbm, a_v),
                (g_own, x_recv.at[x, :, pl.ds(kx, kgx)]),
                (a_own, x_recv.at[x, :, pl.ds(0, kx)]),
                (e_hbm, e_v),
                (q_hbm, q_v),
                (b_hbm.at[:, mine], b_full.at[pl.ds(off, KA), :]),
                (w_hbm.at[:, mine], w_full.at[pl.ds(goff, KG), :]),
                (len_hbm, len_ref),
                (rows_hbm, rows_ref),
                (prior_hbm, prior_ref),
            )
        )
    ]
    for load in loads:
        load.start()

    pl.semaphore_wait(barrier, len(partners) + sec)

    loads[0].wait()
    for k in far_x:
        xx = (x + k) % NX
        send(
            g_v.at[:, pl.ds(pl.multiple_of(kgx * xx, 128), kgx)],
            x_recv.at[x, :, pl.ds(kx, kgx)],
            "x",
            (1, k),
            at(xx, z, c),
        )
    loads[1].wait()
    for k in far_x:
        xx = (x + k) % NX
        send(
            a_v.at[:, pl.ds(pl.multiple_of(kx * xx, 128), kx)],
            x_recv.at[x, :, pl.ds(0, kx)],
            "x",
            (0, k),
            at(xx, z, c),
        )
    twin = at(x, z, 1 - c)
    send(b_hbm.at[:, other], b_full.at[pl.ds(off, KA), :], "bw", (0,), twin)
    send(w_hbm.at[:, other], w_full.at[pl.ds(goff, KG), :], "bw", (1,), twin)

    zero_at = pl.multiple_of((1 - z % 2) * 2 * KA, 64)
    b_full[pl.ds(zero_at, 64), :] = jnp.zeros((64, half), jnp.bfloat16)
    rows_x[...] = jnp.zeros_like(rows_x)
    loads[4].wait()
    loads[5].wait()
    for b in range(2 * NX):
        cols = slice(128 * b, 128 * b + 128)
        den = e_v[:, cols] + DAMPING
        num = q_v[:, :, cols].astype(jnp.float32)
        p_send[b] = (num / den[None]).astype(jnp.bfloat16)
    p_full[2 * x + c] = p_send[4 * c + x]

    loads[2].wait()
    for k in far_x:
        arrived(x_recv.at[(x + NX - k) % NX, :, pl.ds(kx, kgx)], "x", (1, k))
    for zz in range(nz):
        gs = kx + 2 * KG * zz
        z_send_g[zz] = jnp.concatenate(
            [x_recv[i, :, gs : gs + 2 * KG] for i in range(NX)], axis=0
        )
    for k in far_z:
        zz = (z + k) % nz
        send(z_send_g.at[zz], tok_g.at[z, c], "z", (1, k), at(x, zz, c))
    send(z_send_g.at[z], tok_g.at[z, c], "c", (1, 0), twin)
    tok_g[z, c] = z_send_g[z]
    loads[3].wait()
    for k in far_x:
        arrived(x_recv.at[(x + NX - k) % NX, :, pl.ds(0, kx)], "x", (0, k))
    for zz in range(nz):
        start = 896 * (zz // 2) + 384 * (zz % 2)
        z_send_a[zz] = jnp.concatenate(
            [x_recv[i, :, start : start + WIN] for i in range(NX)], axis=0
        )
    for k in far_z:
        zz = (z + k) % nz
        send(z_send_a.at[zz], tok_a.at[z, c], "z", (0, k), at(x, zz, c))
    send(z_send_a.at[z], tok_a.at[z, c], "c", (0, 0), twin)
    tok_a[z, c] = z_send_a[z]
    for i, (dx, dc) in enumerate(group):
        xx, cc = (x + dx) % NX, (c + dc) % 2
        send(p_send.at[4 * cc + xx], p_full.at[2 * x + c], "p", (i,), at(xx, z, cc))

    for k in far_s:

        @pl.when(sec >= k)
        def _(k=k):
            pl.semaphore_signal(ready, inc=1, device_id=(sec - k, dp), device_id_type=MESH)

    loads[6].wait()
    loads[7].wait()
    arrived(w_full.at[pl.ds(goff_twin, KG), :], "bw", (1,))
    w_t[...] = w_full[...].astype(jnp.float32).T.astype(jnp.bfloat16)
    arrived(b_full.at[pl.ds(off_twin, KA), :], "bw", (0,))

    tokens = nz * tz

    def forward(tok, kind, k):
        zz = (z + nz - k) % nz
        arrived(tok.at[zz, c], "z", (kind, k))
        send(tok.at[zz, c], tok.at[zz, c], "c", (kind, k), twin)

    def project_acts(k):
        zz = (z + nz - k) % nz
        arrived(tok_a.at[zz, 1 - c], "c", (0, k))
        part = jnp.dot(
            tok_a[zz].reshape(tz, WIN), b_full[...], preferred_element_type=jnp.float32
        ).astype(jnp.bfloat16)
        for i in range(NX):
            xs_a[zz, i] = part[:, 128 * i : 128 * i + 128]
        for kx_ in far_x:
            xx = (x + kx_) % NX
            send(xs_a.at[zz, xx], xr_a.at[zz, x], "rx", (0, k, kx_), at(xx, z, c))

    def project_grads():
        for k in [0] + near_z:
            arrived(tok_g.at[(z + nz - k) % nz, 1 - c], "c", (1, k))
        part = lax.dot_general(
            w_t[...],
            tok_g[...].reshape(tokens, 2 * KG),
            (((1,), (1,)), ((), ())),
            preferred_element_type=jnp.float32,
        ).astype(jnp.bfloat16)
        for i in range(NX):
            for zz in range(nz):
                r = (i // 2) * 2 * nz * ib + zz * 2 * ib + (i % 2) * ib
                xs_g[zz, i] = part[r : r + ib, :]
        for k in far_z:
            zz = (z + k) % nz
            send(xs_g.at[zz], zr_g.at[z], "rz", (1, k), at(x, zz, c))

    def sum_over_x(own, recv, kind, k):
        total = own.astype(jnp.float32)
        for kx_ in far_x:
            xx = (x + NX - kx_) % NX
            arrived(recv.at[xx], "rx", (kind, k, kx_))
            total = total + recv[xx].astype(jnp.float32)
        return total.astype(jnp.bfloat16)

    def sum_over_z(sums, recv, kind):
        total = sums[z].astype(jnp.float32)
        for k in near_z:
            zz = (z + nz - k) % nz
            arrived(recv.at[zz], "rz", (kind, k))
            total = total + recv[zz].astype(jnp.float32)
        return total.astype(jnp.bfloat16)

    order = [0] + near_z
    for k in near_z:
        forward(tok_g, 1, k)
    for k in near_z:
        forward(tok_a, 0, k)
    project_grads()
    for k in order:
        project_acts(k)

    for k in order:
        zz = (z + nz - k) % nz
        zs_a[zz] = sum_over_x(xs_a[zz, x], xr_a.at[zz], 0, k)
        if k:
            send(zs_a.at[zz], zr_a.at[z], "rz", (0, nz - k), at(x, zz, c))
    zs_g[...] = sum_over_z(xs_g, zr_g, 1)
    for kx_ in far_x:
        xx = (x + kx_) % NX
        send(zs_g.at[xx], xr_g.at[x], "rx", (1, 0, kx_), at(xx, z, c))
    own = sum_over_z(zs_a, zr_a, 0)
    ap_own[...] = own
    for k in far_z:
        send(ap_own, ap_full.at[z], "az", (k,), at(x, (z + k) % nz, c))
    ap_full[z] = own
    own = sum_over_x(zs_g[x], xr_g, 1, 0)
    gp_own[...] = own
    for i, (dx, dc) in enumerate(group):
        xx, cc = (x + dx) % NX, (c + dc) % 2
        send(gp_own, gp_full.at[4 * c + x], "gx", (i,), at(xx, z, cc))
    gp_full[4 * c + x] = own

    for i, (dx, dc) in enumerate(group):
        xx, cc = (x + NX - dx) % NX, (c + 2 - dc) % 2
        arrived(p_full.at[2 * xx + cc], "p", (i,))
        arrived(gp_full.at[4 * cc + xx], "gx", (i,))
    for k in near_z:
        arrived(ap_full.at[(z + nz - k) % nz], "az", (k,))
    for load in loads[8:]:
        load.wait()
    lane = lax.broadcasted_iota(jnp.int32, (8 * ib, tokens), 1)
    micro = lane % 4
    slot = ((lane // 4) % 4) * 2 * nz + (lane // tz) * 2 + (lane // 16) % 2
    gp = gp_full[...].reshape(8 * ib, tokens).astype(jnp.float32)
    ap = ap_full[...].reshape(tokens, 128)
    for m in range(4):
        live = jnp.where(micro == m, slot, 2**20) < len_ref[m]
        seq = jnp.dot(
            jnp.where(live, gp, 0.0).astype(jnp.bfloat16), ap, preferred_element_type=jnp.float32
        )
        for q in range(8):
            row = seq * p_full[:, q].reshape(8 * ib, 128).astype(jnp.float32)
            rows_x[m * 8 + q : m * 8 + q + 1, :] = jnp.sum(row, axis=0, keepdims=True)
    score = lax.dot_general(
        jnp.ones((8, 128), jnp.float32),
        rows_x[...],
        (((1,), (1,)), ((), ())),
        precision=HIGH,
        preferred_element_type=jnp.float32,
    )
    s1_send[...] = score[0:1, :]
    s1_recv[1, 0] = score[0:1, :]
    places = [(dz, dx) for dz in far_z + [0] for dx in (2, 1, 3, 0)]

    def part_copy(dz, dx):
        i = dz * NX + dx
        dev = at((x + dx) % NX, (z + dz) % nz, 1)
        return copy_of(s1_send, s1_recv.at[c, i], "s1", (c, i), dev)

    for dz, dx in places[:-1]:
        copy = part_copy(dz, dx)
        copy.start()
        pending.append(copy)

    @pl.when(c == 0)
    def _():
        part_copy(0, 0).start()

    def score_copy(k):
        return copy_of(s3_send, s3_recv.at[k], "s3", (k,), ((sec + k) % n_sections, dp))

    def twin_copy():
        return copy_of(acc_ref, acc_ref, "fin", (0,), twin)

    @pl.when(sec < n_sections - 1)
    def _():
        pl.semaphore_wait(ready, n_sections - 1 - sec)

    @pl.when(c == 1)
    def _():
        for dz, dx in places[::-1]:
            i = dz * NX + dx
            if i:
                arrived(s1_recv.at[1, i], "s1", (1, i))
            arrived(s1_recv.at[0, i], "s1", (0, i))
        acc = jnp.sum(s1_recv[...].reshape(2 * NX * nz, 1, 128), axis=0)
        s3_send[...] = acc
        for k in far_s:

            @pl.when(sec + k < n_sections)
            def _(k=k):
                score_copy(k).start()

        for k in reversed(far_s):

            @pl.when(sec >= k)
            def _(k=k):
                score_copy(k).wait_recv()

            acc = acc + jnp.where(sec >= k, s3_recv[k], 0.0)
        acc_ref[...] = acc
        twin_copy().start()

    @pl.when(c == 0)
    def _():
        twin_copy().wait_recv()

    acc = acc_ref[...]

    lane = lax.broadcasted_iota(jnp.int32, (8, 128), 1)
    row = lax.broadcasted_iota(jnp.int32, (8, 128), 0) + dp * 8
    length = jnp.full((8, 128), 1, jnp.int32)
    target = jnp.full((8, 128), -1, jnp.int32)
    for m in range(4):
        inside = lane // 8 == m
        length = jnp.where(inside, len_ref[m], length)
        target = jnp.where(inside, rows_ref[m], target)
    scaled = acc * (1.0 / length.astype(jnp.float32))
    spread = jnp.where(target == row, scaled, 0.0)
    pick = lax.broadcasted_iota(jnp.int32, (128, 128), 0) % 8
    pick = pick == lax.broadcasted_iota(jnp.int32, (128, 128), 1)
    table = jnp.dot(
        spread, pick.astype(jnp.float32), precision=HIGH, preferred_element_type=jnp.float32
    )
    out_ref[...] = prior_ref[...] + table[:, 0:8]
    for copy in pending:
        copy.wait_send()

    @pl.when(c == 0)
    def _():
        part_copy(0, 0).wait_send()

    @pl.when(c == 1)
    def _():
        twin_copy().wait_send()
        for k in far_s:

            @pl.when(sec + k < n_sections)
            def _(k=k):
                score_copy(k).wait_send()


def per_device(n_sections, nz, acts, grads, basis_in, basis_out, eig, query, lengths, rows, prior):
    ff, d = acts.shape[3], grads.shape[3]
    rank = basis_in.shape[2]
    half = rank // 2
    ib = eig.shape[1]
    tokens = 2 * nz * 16
    tz = tokens // nz
    kx, kgx = ff // NX, d // NX
    bf, f32 = jnp.bfloat16, jnp.float32
    dma = pltpu.SemaphoreType.DMA
    vm = pltpu.VMEM
    hbm = pl.BlockSpec(memory_space=pl.ANY)
    vmem = pl.BlockSpec(memory_space=pltpu.VMEM)
    out = pl.pallas_call(
        functools.partial(kernel, n_sections, nz),
        out_shape=jax.ShapeDtypeStruct(prior.shape, f32),
        in_specs=[hbm] * 9,
        out_specs=vmem,
        scratch_shapes=[
            pltpu.SMEM((4,), jnp.int32),
            pltpu.SMEM((4,), jnp.int32),
            vm(prior.shape, f32),
            vm((4, ff), bf),
            vm((4, d), bf),
            vm((ib, rank), f32),
            vm((8, ib, rank), bf),
            vm((WIN, half), bf),
            vm((2 * KG, half), bf),
            vm((half, 2 * KG), bf),
            vm((2 * NX, 8, ib, 128), bf),
            vm((2 * NX, 8, ib, 128), bf),
            vm((NX, 4, kx + kgx), bf),
            vm((nz, 16, WIN), bf),
            vm((nz, 16, 2 * KG), bf),
            vm((nz, 2, 16, WIN), bf),
            vm((nz, 2, 16, 2 * KG), bf),
            vm((nz, NX, tz, 128), bf),
            vm((nz, NX, ib, tokens), bf),
            vm((nz, NX, tz, 128), bf),
            vm((NX, ib, tokens), bf),
            vm((nz, tz, 128), bf),
            vm((NX, ib, tokens), bf),
            vm((nz, tz, 128), bf),
            vm((nz, NX, ib, tokens), bf),
            vm((tz, 128), bf),
            vm((ib, tokens), bf),
            vm((nz, tz, 128), bf),
            vm((2 * NX, ib, tokens), bf),
            vm((128, 128), f32),
            vm((1, 128), f32),
            vm((2, NX * nz, 1, 128), f32),
            vm((1, 128), f32),
            vm((n_sections, 1, 128), f32),
            vm((1, 128), f32),
            dma((11,)),
            pltpu.SemaphoreType.REGULAR,
            dma((2, 2, NX)),
            dma((2, 2, nz)),
            dma((2, 2, nz)),
            dma((2, 2)),
            dma((2, 7)),
            dma((2, 2, nz, NX)),
            dma((2, 2, nz)),
            dma((2, nz)),
            dma((2, 7)),
            dma((2, 2, NX * nz)),
            dma((2, n_sections)),
            dma((2, 1)),
        ],
        compiler_params=pltpu.CompilerParams(collective_id=0, has_side_effects=True),
    )(
        acts.reshape(4, ff),
        grads.reshape(4, d),
        basis_in[0],
        basis_out[0],
        eig[0],
        query[0],
        lengths,
        rows,
        prior,
    )
    return out[None]


def solution(mesh):
    n_sections, n_dp = mesh.shape["section"], mesh.shape["dp"]
    return jax.shard_map(
        functools.partial(per_device, n_sections, n_dp // (NX * NC)),
        mesh=mesh,
        in_specs=(
            P("section", None, "dp", None),
            P("section", None, "dp", None),
            P("section", "dp", None),
            P("section", "dp", None),
            P("section", "dp", None),
            P("section", None, "dp", None),
            P(),
            P(),
            P("dp", None),
        ),
        out_specs=P("section", "dp", None),
        check_vma=False,
    )
```

```python
import functools

import jax
import jax.numpy as jnp
from jax import lax
from jax.experimental import pallas as pl
from jax.experimental.pallas import tpu as pltpu
from jax.sharding import PartitionSpec as P

DAMPING = 0.01
MESH = pl.DeviceIdType.MESH
NX = 4
NC = 2
KA = 224
KG = 64
WIN = 512
SEMS = ("x", "z", "c", "bw", "p", "rx", "rz", "az", "gx", "s1", "s3", "fin")
HIGH = lax.Precision.HIGHEST


def far_first(n):
    return sorted(range(1, n), key=lambda k: -min(k, n - k))


def kernel(
    n_sections,
    nz,
    a_hbm,
    g_hbm,
    b_hbm,
    w_hbm,
    e_hbm,
    q_hbm,
    len_hbm,
    rows_hbm,
    prior_hbm,
    out_ref,
    len_ref,
    rows_ref,
    prior_ref,
    a_v,
    g_v,
    e_v,
    q_v,
    b_full,
    w_full,
    w_t,
    p_send,
    p_full,
    x_recv,
    z_send_a,
    z_send_g,
    tok_a,
    tok_g,
    xs_a,
    xs_g,
    xr_a,
    xr_g,
    zs_a,
    zs_g,
    zr_a,
    zr_g,
    ap_own,
    gp_own,
    ap_full,
    gp_full,
    rows_x,
    s1_send,
    s1_recv,
    s3_send,
    s3_recv,
    acc_ref,
    load_sem,
    ready,
    *sem_refs,
):
    sec = lax.axis_index("section")
    dp = lax.axis_index("dp")
    x = dp // (2 * nz)
    z = (dp % (2 * nz)) // 2
    c = dp % 2
    ib = gp_own.shape[0]
    tz = ap_own.shape[0]
    half = w_full.shape[1]
    kgx = nz * 2 * KG
    kx = x_recv.shape[2] - kgx
    sems = dict(zip(SEMS, sem_refs, strict=True))

    def at(xx, zz, cc):
        return (sec, (xx * nz + zz) * 2 + cc)

    def copy_of(src, dst, name, i, dev):
        return pltpu.make_async_remote_copy(
            src_ref=src,
            dst_ref=dst,
            send_sem=sems[name].at[(0, *i)],
            recv_sem=sems[name].at[(1, *i)],
            device_id=dev,
            device_id_type=MESH,
        )

    def send(src, dst, name, i, dev):
        copy = copy_of(src, dst, name, i, dev)
        copy.start()
        pending.append(copy)

    def arrived(dst, name, i):
        copy_of(dst, dst, name, i, (sec, dp)).wait_recv()

    pending = []
    far_x = far_first(NX)
    far_z = far_first(nz)
    near_z = far_z[::-1]
    far_s = far_first(n_sections)
    group = [(dx, dc) for dx in (2, 1, 3, 0) for dc in (0, 1) if dx or dc]

    barrier = pltpu.get_barrier_semaphore()
    partners = [at((x + dx) % NX, z, (c + dc) % 2) for dx, dc in group]
    partners += [at(x, (z + k) % nz, c) for k in far_z]
    for dev in partners:
        pl.semaphore_signal(barrier, inc=1, device_id=dev, device_id_type=MESH)
    for k in far_s:

        @pl.when(sec + k < n_sections)
        def _(k=k):
            pl.semaphore_signal(barrier, inc=1, device_id=(sec + k, dp), device_id_type=MESH)

    off = pl.multiple_of(64 * (z % 2) + KA * c, 32)
    off_twin = pl.multiple_of(64 * (z % 2) + KA * (1 - c), 32)
    goff = pl.multiple_of(KG * c, 64)
    goff_twin = pl.multiple_of(KG * (1 - c), 64)
    mine = pl.ds(pl.multiple_of(half * c, 128), half)
    other = pl.ds(pl.multiple_of(half * (1 - c), 128), half)
    a_own = a_hbm.at[:, pl.ds(pl.multiple_of(kx * x, 128), kx)]
    g_own = g_hbm.at[:, pl.ds(pl.multiple_of(kgx * x, 128), kgx)]
    loads = [
        pltpu.make_async_copy(s, d, load_sem.at[i])
        for i, (s, d) in enumerate(
            (
                (g_hbm, g_v),
                (a_hbm, a_v),
                (g_own, x_recv.at[x, :, pl.ds(kx, kgx)]),
                (a_own, x_recv.at[x, :, pl.ds(0, kx)]),
                (e_hbm, e_v),
                (q_hbm, q_v),
                (b_hbm.at[:, mine], b_full.at[pl.ds(off, KA), :]),
                (w_hbm.at[:, mine], w_full.at[pl.ds(goff, KG), :]),
                (len_hbm, len_ref),
                (rows_hbm, rows_ref),
                (prior_hbm, prior_ref),
            )
        )
    ]
    for load in loads:
        load.start()

    pl.semaphore_wait(barrier, len(partners) + sec)

    loads[0].wait()
    for k in far_x:
        xx = (x + k) % NX
        send(
            g_v.at[:, pl.ds(pl.multiple_of(kgx * xx, 128), kgx)],
            x_recv.at[x, :, pl.ds(kx, kgx)],
            "x",
            (1, k),
            at(xx, z, c),
        )
    loads[1].wait()
    for k in far_x:
        xx = (x + k) % NX
        send(
            a_v.at[:, pl.ds(pl.multiple_of(kx * xx, 128), kx)],
            x_recv.at[x, :, pl.ds(0, kx)],
            "x",
            (0, k),
            at(xx, z, c),
        )
    twin = at(x, z, 1 - c)
    send(b_hbm.at[:, other], b_full.at[pl.ds(off, KA), :], "bw", (0,), twin)
    send(w_hbm.at[:, other], w_full.at[pl.ds(goff, KG), :], "bw", (1,), twin)

    zero_at = pl.multiple_of((1 - z % 2) * 2 * KA, 64)
    b_full[pl.ds(zero_at, 64), :] = jnp.zeros((64, half), jnp.bfloat16)
    rows_x[...] = jnp.zeros_like(rows_x)
    loads[4].wait()
    loads[5].wait()
    for b in range(2 * NX):
        cols = slice(128 * b, 128 * b + 128)
        den = e_v[:, cols] + DAMPING
        num = q_v[:, :, cols].astype(jnp.float32)
        p_send[b] = (num / den[None]).astype(jnp.bfloat16)
    p_full[2 * x + c] = p_send[4 * c + x]

    loads[2].wait()
    for k in far_x:
        arrived(x_recv.at[(x + NX - k) % NX, :, pl.ds(kx, kgx)], "x", (1, k))
    for zz in range(nz):
        gs = kx + 2 * KG * zz
        z_send_g[zz] = jnp.concatenate(
            [x_recv[i, :, gs : gs + 2 * KG] for i in range(NX)], axis=0
        )
    for k in far_z:
        zz = (z + k) % nz
        send(z_send_g.at[zz], tok_g.at[z, c], "z", (1, k), at(x, zz, c))
    send(z_send_g.at[z], tok_g.at[z, c], "c", (1, 0), twin)
    tok_g[z, c] = z_send_g[z]
    loads[3].wait()
    for k in far_x:
        arrived(x_recv.at[(x + NX - k) % NX, :, pl.ds(0, kx)], "x", (0, k))
    for zz in range(nz):
        start = 896 * (zz // 2) + 384 * (zz % 2)
        z_send_a[zz] = jnp.concatenate(
            [x_recv[i, :, start : start + WIN] for i in range(NX)], axis=0
        )
    for k in far_z:
        zz = (z + k) % nz
        send(z_send_a.at[zz], tok_a.at[z, c], "z", (0, k), at(x, zz, c))
    send(z_send_a.at[z], tok_a.at[z, c], "c", (0, 0), twin)
    tok_a[z, c] = z_send_a[z]
    for i, (dx, dc) in enumerate(group):
        xx, cc = (x + dx) % NX, (c + dc) % 2
        send(p_send.at[4 * cc + xx], p_full.at[2 * x + c], "p", (i,), at(xx, z, cc))

    for k in far_s:

        @pl.when(sec >= k)
        def _(k=k):
            pl.semaphore_signal(ready, inc=1, device_id=(sec - k, dp), device_id_type=MESH)

    loads[6].wait()
    loads[7].wait()
    arrived(w_full.at[pl.ds(goff_twin, KG), :], "bw", (1,))
    w_t[...] = w_full[...].astype(jnp.float32).T.astype(jnp.bfloat16)
    arrived(b_full.at[pl.ds(off_twin, KA), :], "bw", (0,))

    tokens = nz * tz

    def forward(tok, kind, k):
        zz = (z + nz - k) % nz
        arrived(tok.at[zz, c], "z", (kind, k))
        send(tok.at[zz, c], tok.at[zz, c], "c", (kind, k), twin)

    def project_acts(k):
        zz = (z + nz - k) % nz
        arrived(tok_a.at[zz, 1 - c], "c", (0, k))
        part = jnp.dot(
            tok_a[zz].reshape(tz, WIN), b_full[...], preferred_element_type=jnp.float32
        ).astype(jnp.bfloat16)
        for i in range(NX):
            xs_a[zz, i] = part[:, 128 * i : 128 * i + 128]
        for kx_ in far_x:
            xx = (x + kx_) % NX
            send(xs_a.at[zz, xx], xr_a.at[zz, x], "rx", (0, k, kx_), at(xx, z, c))

    def project_grads():
        for k in [0] + near_z:
            arrived(tok_g.at[(z + nz - k) % nz, 1 - c], "c", (1, k))
        part = lax.dot_general(
            w_t[...],
            tok_g[...].reshape(tokens, 2 * KG),
            (((1,), (1,)), ((), ())),
            preferred_element_type=jnp.float32,
        ).astype(jnp.bfloat16)
        for i in range(NX):
            for zz in range(nz):
                r = (i // 2) * 2 * nz * ib + zz * 2 * ib + (i % 2) * ib
                xs_g[zz, i] = part[r : r + ib, :]
        for k in far_z:
            zz = (z + k) % nz
            send(xs_g.at[zz], zr_g.at[z], "rz", (1, k), at(x, zz, c))

    def sum_over_x(own, recv, kind, k):
        total = own.astype(jnp.float32)
        for kx_ in far_x:
            xx = (x + NX - kx_) % NX
            arrived(recv.at[xx], "rx", (kind, k, kx_))
            total = total + recv[xx].astype(jnp.float32)
        return total.astype(jnp.bfloat16)

    def sum_over_z(sums, recv, kind):
        total = sums[z].astype(jnp.float32)
        for k in near_z:
            zz = (z + nz - k) % nz
            arrived(recv.at[zz], "rz", (kind, k))
            total = total + recv[zz].astype(jnp.float32)
        return total.astype(jnp.bfloat16)

    order = [0] + near_z
    for k in near_z:
        forward(tok_g, 1, k)
    for k in near_z:
        forward(tok_a, 0, k)
    project_grads()
    for k in order:
        project_acts(k)

    for k in order:
        zz = (z + nz - k) % nz
        zs_a[zz] = sum_over_x(xs_a[zz, x], xr_a.at[zz], 0, k)
        if k:
            send(zs_a.at[zz], zr_a.at[z], "rz", (0, nz - k), at(x, zz, c))
    zs_g[...] = sum_over_z(xs_g, zr_g, 1)
    for kx_ in far_x:
        xx = (x + kx_) % NX
        send(zs_g.at[xx], xr_g.at[x], "rx", (1, 0, kx_), at(xx, z, c))
    own = sum_over_z(zs_a, zr_a, 0)
    ap_own[...] = own
    for k in far_z:
        send(ap_own, ap_full.at[z], "az", (k,), at(x, (z + k) % nz, c))
    ap_full[z] = own
    own = sum_over_x(zs_g[x], xr_g, 1, 0)
    gp_own[...] = own
    for i, (dx, dc) in enumerate(group):
        xx, cc = (x + dx) % NX, (c + dc) % 2
        send(gp_own, gp_full.at[4 * c + x], "gx", (i,), at(xx, z, cc))
    gp_full[4 * c + x] = own

    for i, (dx, dc) in enumerate(group):
        xx, cc = (x + NX - dx) % NX, (c + 2 - dc) % 2
        arrived(p_full.at[2 * xx + cc], "p", (i,))
        arrived(gp_full.at[4 * cc + xx], "gx", (i,))
    for k in near_z:
        arrived(ap_full.at[(z + nz - k) % nz], "az", (k,))
    for load in loads[8:]:
        load.wait()
    lane = lax.broadcasted_iota(jnp.int32, (8 * ib, tokens), 1)
    micro = lane % 4
    slot = ((lane // 4) % 4) * 2 * nz + (lane // tz) * 2 + (lane // 16) % 2
    gp = gp_full[...].reshape(8 * ib, tokens).astype(jnp.float32)
    ap = ap_full[...].reshape(tokens, 128)
    for m in range(4):
        live = jnp.where(micro == m, slot, 2**20) < len_ref[m]
        seq = jnp.dot(
            jnp.where(live, gp, 0.0).astype(jnp.bfloat16), ap, preferred_element_type=jnp.float32
        )
        for q in range(8):
            row = seq * p_full[:, q].reshape(8 * ib, 128).astype(jnp.float32)
            rows_x[m * 8 + q : m * 8 + q + 1, :] = jnp.sum(row, axis=0, keepdims=True)
    score = lax.dot_general(
        jnp.ones((8, 128), jnp.float32),
        rows_x[...],
        (((1,), (1,)), ((), ())),
        precision=HIGH,
        preferred_element_type=jnp.float32,
    )
    s1_send[...] = score[0:1, :]
    s1_recv[1, 0] = score[0:1, :]
    places = [(dz, dx) for dz in far_z + [0] for dx in (2, 1, 3, 0)]

    def part_copy(dz, dx):
        i = dz * NX + dx
        dev = at((x + dx) % NX, (z + dz) % nz, 1)
        return copy_of(s1_send, s1_recv.at[c, i], "s1", (c, i), dev)

    for dz, dx in places[:-1]:
        copy = part_copy(dz, dx)
        copy.start()
        pending.append(copy)

    @pl.when(c == 0)
    def _():
        part_copy(0, 0).start()

    def score_copy(k):
        return copy_of(s3_send, s3_recv.at[k], "s3", (k,), ((sec + k) % n_sections, dp))

    def twin_copy():
        return copy_of(acc_ref, acc_ref, "fin", (0,), twin)

    @pl.when(sec < n_sections - 1)
    def _():
        pl.semaphore_wait(ready, n_sections - 1 - sec)

    @pl.when(c == 1)
    def _():
        for dz, dx in places[::-1]:
            i = dz * NX + dx
            if i:
                arrived(s1_recv.at[1, i], "s1", (1, i))
            arrived(s1_recv.at[0, i], "s1", (0, i))
        acc = jnp.sum(s1_recv[...].reshape(2 * NX * nz, 1, 128), axis=0)
        s3_send[...] = acc
        for k in far_s:

            @pl.when(sec + k < n_sections)
            def _(k=k):
                score_copy(k).start()

        for k in reversed(far_s):

            @pl.when(sec >= k)
            def _(k=k):
                score_copy(k).wait_recv()

            acc = acc + jnp.where(sec >= k, s3_recv[k], 0.0)
        acc_ref[...] = acc
        twin_copy().start()

    @pl.when(c == 0)
    def _():
        twin_copy().wait_recv()

    acc = acc_ref[...]

    lane = lax.broadcasted_iota(jnp.int32, (8, 128), 1)
    row = lax.broadcasted_iota(jnp.int32, (8, 128), 0) + dp * 8
    length = jnp.full((8, 128), 1, jnp.int32)
    target = jnp.full((8, 128), -1, jnp.int32)
    for m in range(4):
        inside = lane // 8 == m
        length = jnp.where(inside, len_ref[m], length)
        target = jnp.where(inside, rows_ref[m], target)
    scaled = acc * (1.0 / length.astype(jnp.float32))
    spread = jnp.where(target == row, scaled, 0.0)
    pick = lax.broadcasted_iota(jnp.int32, (128, 128), 0) % 8
    pick = pick == lax.broadcasted_iota(jnp.int32, (128, 128), 1)
    table = jnp.dot(
        spread, pick.astype(jnp.float32), precision=HIGH, preferred_element_type=jnp.float32
    )
    out_ref[...] = prior_ref[...] + table[:, 0:8]
    for copy in pending:
        copy.wait_send()

    @pl.when(c == 0)
    def _():
        part_copy(0, 0).wait_send()

    @pl.when(c == 1)
    def _():
        twin_copy().wait_send()
        for k in far_s:

            @pl.when(sec + k < n_sections)
            def _(k=k):
                score_copy(k).wait_send()


def per_device(n_sections, nz, acts, grads, basis_in, basis_out, eig, query, lengths, rows, prior):
    ff, d = acts.shape[3], grads.shape[3]
    rank = basis_in.shape[2]
    half = rank // 2
    ib = eig.shape[1]
    tokens = 2 * nz * 16
    tz = tokens // nz
    kx, kgx = ff // NX, d // NX
    bf, f32 = jnp.bfloat16, jnp.float32
    dma = pltpu.SemaphoreType.DMA
    vm = pltpu.VMEM
    hbm = pl.BlockSpec(memory_space=pl.ANY)
    vmem = pl.BlockSpec(memory_space=pltpu.VMEM)
    out = pl.pallas_call(
        functools.partial(kernel, n_sections, nz),
        out_shape=pltpu.VMEM(prior.shape, f32),
        in_specs=[hbm] * 9,
        out_specs=vmem,
        scratch_shapes=[
            pltpu.SMEM((4,), jnp.int32),
            pltpu.SMEM((4,), jnp.int32),
            vm(prior.shape, f32),
            vm((4, ff), bf),
            vm((4, d), bf),
            vm((ib, rank), f32),
            vm((8, ib, rank), bf),
            vm((WIN, half), bf),
            vm((2 * KG, half), bf),
            vm((half, 2 * KG), bf),
            vm((2 * NX, 8, ib, 128), bf),
            vm((2 * NX, 8, ib, 128), bf),
            vm((NX, 4, kx + kgx), bf),
            vm((nz, 16, WIN), bf),
            vm((nz, 16, 2 * KG), bf),
            vm((nz, 2, 16, WIN), bf),
            vm((nz, 2, 16, 2 * KG), bf),
            vm((nz, NX, tz, 128), bf),
            vm((nz, NX, ib, tokens), bf),
            vm((nz, NX, tz, 128), bf),
            vm((NX, ib, tokens), bf),
            vm((nz, tz, 128), bf),
            vm((NX, ib, tokens), bf),
            vm((nz, tz, 128), bf),
            vm((nz, NX, ib, tokens), bf),
            vm((tz, 128), bf),
            vm((ib, tokens), bf),
            vm((nz, tz, 128), bf),
            vm((2 * NX, ib, tokens), bf),
            vm((128, 128), f32),
            vm((1, 128), f32),
            vm((2, NX * nz, 1, 128), f32),
            vm((1, 128), f32),
            vm((n_sections, 1, 128), f32),
            vm((1, 128), f32),
            dma((11,)),
            pltpu.SemaphoreType.REGULAR,
            dma((2, 2, NX)),
            dma((2, 2, nz)),
            dma((2, 2, nz)),
            dma((2, 2)),
            dma((2, 7)),
            dma((2, 2, nz, NX)),
            dma((2, 2, nz)),
            dma((2, nz)),
            dma((2, 7)),
            dma((2, 2, NX * nz)),
            dma((2, n_sections)),
            dma((2, 1)),
        ],
        compiler_params=pltpu.CompilerParams(collective_id=0, has_side_effects=True),
    )(
        acts.reshape(4, ff),
        grads.reshape(4, d),
        basis_in[0],
        basis_out[0],
        eig[0],
        query[0],
        lengths,
        rows,
        prior,
    )
    return out[None]


def solution(mesh):
    n_sections, n_dp = mesh.shape["section"], mesh.shape["dp"]
    return jax.shard_map(
        functools.partial(per_device, n_sections, n_dp // (NX * NC)),
        mesh=mesh,
        in_specs=(
            P("section", None, "dp", None),
            P("section", None, "dp", None),
            P("section", "dp", None),
            P("section", "dp", None),
            P("section", "dp", None),
            P("section", None, "dp", None),
            P(),
            P(),
            P("dp", None),
        ),
        out_specs=P("section", "dp", None),
        check_vma=False,
    )
```
